128 devices in a mesh: dp: 64 (over z, y, x), mp: 2 (over core).
Axes of the slice: x: 4, y: 4, z: 4, core: 2. Of those that a mesh axis runs over, the one named last changes fastest.
Arguments:
- hot_rows: int32 [64, 64, 32], P('dp'), may hold values from 0 to 4095
- hot_count: int32 [64, 64], P('dp'), may hold values from 1 to 32, as said below
- hot_cot: bfloat16 [64, 64, 32, 128], P('dp'), may hold values from -6 to 6
- table: float32 [262144, 128], P('dp'), may hold values from -3 to 3
- cold_ids: int32 [65536], P('dp'), may hold values from 0 to 1048575
- hash_mult: int32 [1024], replicated, may hold values from 1 to 1023
- hash_add: int32 [1024], replicated, may hold values from 0 to 1000002
- layer_one: bfloat16 [1024, 1024], P(None, 'mp'), may hold values from -0.1875 to 0.1875
- layer_two: bfloat16 [1024, 1024], P('mp'), may hold values from -0.1875 to 0.1875
- layer_three: bfloat16 [1024, 1024], P(None, 'mp'), may hold values from -0.1875 to 0.1875
- layer_four: bfloat16 [1024, 128], P('mp'), may hold values from -0.1875 to 0.1875
- cold_cot: bfloat16 [65536, 128], P('dp'), may hold values from -6 to 6
Outputs:
- hot_emb: bfloat16 [64, 64, 32, 128], P('dp')
- new_table: float32 [262144, 128], P('dp')
- cold_emb: bfloat16 [65536, 128], P('dp')
- grad_one: float32 [1024, 1024], P(None, 'mp')
- grad_two: float32 [1024, 1024], P('mp')
- grad_three: float32 [1024, 1024], P(None, 'mp')
- grad_four: float32 [1024, 128], P('mp')
The draws below stay inside these ranges and needn't reach their ends.
Inputs may be any that keep to these rules, and one draw needn't show every extreme that they name: `hot_rows`: entries index the owner's block of 4096 rows; entries in unused slots are arbitrary. `hot_count`: every batch shard fills all 32 slots of some owner, and some owner receives 32 from every batch shard.
All inputs are finite; a program needn't handle non-finite values.
Results may differ from the reference program's by a relative error of at most 0.0074.
Values may be sent and summed in bfloat16 or wider, within the bound.
A program may use at most 128 MiB of HBM per device.

```python
import jax
import jax.numpy as jnp

E = 128
F = 1024
H = 1024
HOT_DEV = 4096
CAP = 32
HOT = 262144
COLDS = 65536
N_DP = 64


def draw_hot_count(key, part):
    first = jax.random.fold_in(key, 11)
    second = jax.random.fold_in(key, 12)
    third = jax.random.fold_in(key, 13)
    counts = jax.random.randint(first, (N_DP, N_DP), 1, CAP + 1)
    own_full = jax.random.randint(second, (N_DP, 1), 0, N_DP)
    common = jax.random.randint(third, (), 0, N_DP)
    columns = jnp.arange(N_DP)[None, :]
    filled = (columns == own_full) | (columns == common)
    return jnp.where(filled, CAP, counts).astype(jnp.int32)


def place_ends(entries, own_key, least, top_value):
    longest = entries.shape.index(max(entries.shape))
    spots = []
    for shift in (0, 1):
        where = [jax.random.randint(jax.random.fold_in(own_key, axis), (), 0, length) for axis, length in enumerate(entries.shape)]
        where[longest] = (where[longest] + shift) % entries.shape[longest]
        spots.append(tuple(where))
    return entries.at[spots[0]].set(least).at[spots[1]].set(top_value)


def shard_levels(rng, shape, cuts, smallest, top_value):
    loudness, own = 1.0, jax.random.fold_in(rng, 6)
    for position, shards_of in cuts:
        steps = jnp.exp(jax.random.uniform(jax.random.fold_in(own, position), (shards_of,), jnp.float32, smallest / len(cuts), top_value / len(cuts)))
        loudness = loudness * jnp.repeat(steps, shape[position] // shards_of).reshape([-1 if axis == position else 1 for axis in range(len(shape))])
    return loudness


def scatter_about(stream_key, shape, deviation, limit, shards=(), kind=jnp.bfloat16):
    values = deviation * jax.random.normal(stream_key, shape, jnp.float32)
    if shards:
        values = values * shard_levels(stream_key, shape, shards, -0.22, 0.18)
    return jnp.clip(values, -limit, limit).astype(kind)


def setup_inputs(seed: int = 0) -> dict:
    arg_keys = jax.random.split(jax.random.key(seed), 13)
    hot_rows = place_ends(jax.random.randint(arg_keys[0], (N_DP, N_DP, CAP), 0, HOT_DEV), jax.random.fold_in(arg_keys[0], 1), 0, HOT_DEV - 1).astype(jnp.int32)
    hot_count = draw_hot_count(jax.random.fold_in(arg_keys[12], 71), 0)
    hot_cot = scatter_about(arg_keys[2], (N_DP, N_DP, CAP, E), 1.0, 6.0, ((0, 64),))
    table = scatter_about(arg_keys[3], (HOT, E), 0.5, 3.0, ((0, 64),), jnp.float32)
    cold_ids = place_ends(jax.random.randint(arg_keys[4], (COLDS,), 0, 1048576), jax.random.fold_in(arg_keys[4], 1), 0, 1048575).astype(jnp.int32)
    hash_mult = place_ends(jax.random.randint(arg_keys[5], (F,), 1, 1024), jax.random.fold_in(arg_keys[5], 1), 1, 1023).astype(jnp.int32)
    hash_add = place_ends(jax.random.randint(arg_keys[6], (F,), 0, 1000003), jax.random.fold_in(arg_keys[6], 1), 0, 1000002).astype(jnp.int32)
    layer_one = scatter_about(arg_keys[7], (F, H), F ** -0.5, 0.1875, ((1, 2),))
    layer_two = scatter_about(arg_keys[8], (H, H), H ** -0.5, 0.1875, ((0, 2),))
    layer_three = scatter_about(arg_keys[9], (H, H), H ** -0.5, 0.1875, ((1, 2),))
    layer_four = scatter_about(arg_keys[10], (H, E), H ** -0.5, 0.1875, ((0, 2),))
    cold_cot = scatter_about(arg_keys[11], (COLDS, E), 1.0, 6.0, ((0, 64),))
    return dict(hot_rows=hot_rows, hot_count=hot_count, hot_cot=hot_cot, table=table, cold_ids=cold_ids, hash_mult=hash_mult, hash_add=hash_add, layer_one=layer_one, layer_two=layer_two, layer_three=layer_three, layer_four=layer_four, cold_cot=cold_cot)


learn_rate = 0.5
modulus = 1000003

def features_of(ids, hash_mult, hash_add):
    hashed = jnp.remainder(ids[:, None] * hash_mult[None, :] + hash_add[None, :], modulus)
    return (hashed.astype(jnp.float32) * (2.0 / 1000002.0) - 1.0).astype(jnp.bfloat16)

def silu_grad(value):
    sig = jax.nn.sigmoid(value)
    return sig * (1.0 + value * (1.0 - sig))

def reference(hot_rows, hot_count, hot_cot, table, cold_ids, hash_mult, hash_add, layer_one, layer_two, layer_three, layer_four, cold_cot):
    slots = jnp.arange(CAP, dtype=jnp.int32)
    used = slots[None, None, :] < hot_count[:, :, None]
    owners = jnp.arange(N_DP, dtype=jnp.int32)[None, :, None] * HOT_DEV
    row = (owners + hot_rows).astype(jnp.int32)
    hot_emb = jnp.where(used[..., None], table[row], 0.0).astype(jnp.bfloat16)
    masked = jnp.where(used[..., None], hot_cot.astype(jnp.float32), 0.0)
    table_grad = jnp.zeros_like(table).at[row.reshape(-1)].add(masked.reshape(-1, E))
    new_table = table - learn_rate * table_grad
    feats = features_of(cold_ids, hash_mult, hash_add)
    pre_one = jnp.dot(feats, layer_one, preferred_element_type=jnp.float32)
    act_one = jax.nn.silu(pre_one).astype(jnp.bfloat16)
    pre_two = jnp.dot(act_one, layer_two, preferred_element_type=jnp.float32)
    act_two = jax.nn.silu(pre_two).astype(jnp.bfloat16)
    pre_three = jnp.dot(act_two, layer_three, preferred_element_type=jnp.float32)
    act_three = jax.nn.silu(pre_three).astype(jnp.bfloat16)
    cold_emb = jnp.dot(act_three, layer_four, preferred_element_type=jnp.float32).astype(jnp.bfloat16)
    back_three = (jnp.dot(cold_cot, layer_four.T, preferred_element_type=jnp.float32) * silu_grad(pre_three)).astype(jnp.bfloat16)
    back_two = (jnp.dot(back_three, layer_three.T, preferred_element_type=jnp.float32) * silu_grad(pre_two)).astype(jnp.bfloat16)
    back_one = (jnp.dot(back_two, layer_two.T, preferred_element_type=jnp.float32) * silu_grad(pre_one)).astype(jnp.bfloat16)
    factor = float(COLDS) ** (-0.5)
    grad_four = jnp.dot(act_three.T, cold_cot, preferred_element_type=jnp.float32) * factor
    grad_three = jnp.dot(act_two.T, back_three, preferred_element_type=jnp.float32) * factor
    grad_two = jnp.dot(act_one.T, back_two, preferred_element_type=jnp.float32) * factor
    grad_one = jnp.dot(feats.T, back_one, preferred_element_type=jnp.float32) * factor
    return (hot_emb, new_table, cold_emb, grad_one, grad_two, grad_three, grad_four)
```

```python
import functools

import jax
import jax.numpy as jnp
from jax import lax
from jax.experimental import pallas as pl
from jax.experimental.pallas import tpu as pltpu
from jax.sharding import PartitionSpec as P

MESH = pl.DeviceIdType.MESH
learn_rate = 0.5
modulus = 1000003
RING = 4
PLANE = RING * RING
CHUNKS = RING * PLANE

STREAMS = (
    (0, 0, 2, 0),
    (0, 2, 1, 1),
    (0, 3, 1, 2),
    (1, 0, 1, 1),
    (2, 0, 2, 1),
    (2, 2, 1, 2),
    (2, 3, 1, 0),
    (3, 0, 2, 2),
    (3, 2, 1, 0),
    (3, 3, 1, 1),
)
BLOCKS = (4, 1, 4, 4)
ROWS = (16, 8, 16, 16)
TYPES = (jnp.bfloat16, jnp.float32, jnp.bfloat16, jnp.bfloat16)
HALF = PLANE // 2


class Place:
    def __init__(self, axis):
        me = lax.axis_index("dp")
        self.core = lax.axis_index("mp")
        strides = (1, RING, RING * RING)
        self.stride = strides[axis]
        self.others = (strides[(axis + 1) % 3], strides[(axis + 2) % 3])
        self.k = lax.rem(me // self.stride, RING)
        self.first = lax.rem(me // self.others[0], RING)
        self.second = lax.rem(me // self.others[1], RING)
        self.p = self.first * RING + self.second
        self.after = lax.rem(self.k + 1, RING)
        self.before = lax.rem(self.k + RING - 1, RING)
        self.opposite = lax.rem(self.k + 2, RING)
        self.right = me + (self.after - self.k) * self.stride
        self.left = me + (self.before - self.k) * self.stride

    def peer(self, p):
        return (
            self.k * self.stride
            + (p // RING) * self.others[0]
            + lax.rem(p, RING) * self.others[1]
        )


class Stream:
    def __init__(self, index, refs, place):
        self.grad, self.b0, self.nb, axis = STREAMS[index]
        self.place = place[axis]
        self.index = index
        g = self.grad
        blocks = pl.ds(self.b0, self.nb)
        self.own = refs["own"][g].at[blocks]
        self.other = refs["other"][g].at[blocks]
        self.arrive = refs["arrive"][g].at[blocks]
        self.total = refs["total"][g].at[blocks]
        self.out = refs["out"][g].at[blocks]
        self.near = refs["near"][g].at[blocks]
        self.side = refs["side"][g].at[blocks]
        self.part = refs["part"][g].at[blocks]
        self.fan = refs["fan"][g].at[blocks]
        self.final = refs["final"][g].at[blocks]
        self.send = refs["send"]
        self.recv = refs["recv"]
        self.dtype = TYPES[g]
        self.pending = []

    def sems(self, slot):
        return self.send.at[self.index, slot], self.recv.at[self.index, slot]

    def copy(self, src, dst, slot, device):
        s, r = self.sems(slot)
        return pltpu.make_async_remote_copy(
            src_ref=src, dst_ref=dst, send_sem=s, recv_sem=r,
            device_id=device, device_id_type=MESH,
        )

    def start(self, src, dst, slot, dp=None, mp=None):
        where = (
            lax.axis_index("dp") if dp is None else dp,
            self.place.core if mp is None else mp,
        )
        c = self.copy(src, dst, slot, where)
        c.start()
        self.pending.append(c)
        return c

    def swap(self):
        self.c_swap = self.start(self.other, self.arrive, 0, mp=1 - self.place.core)

    def chunk(self, ref, first, count):
        return ref.at[:, pl.ds(first, count)]

    def combine(self):
        self.c_swap.wait_recv()

        @pl.loop(0, CHUNKS // 2)
        def _(i):
            rows = pl.ds(i * 2, 2)
            self.total[:, rows] = (
                self.own[:, rows].astype(jnp.float32)
                + self.arrive[:, rows].astype(jnp.float32)
            ).astype(self.dtype)

        q = self.place
        base = q.opposite * PLANE
        self.c_na = self.start(
            self.chunk(self.total, base, HALF), self.chunk(self.near, 0, HALF), 1, dp=q.right
        )
        self.c_nb = self.start(
            self.chunk(self.total, base + HALF, HALF), self.chunk(self.near, HALF, HALF), 2, dp=q.left
        )
        self.c_sa = self.start(
            self.chunk(self.total, q.after * PLANE + HALF, HALF),
            self.chunk(self.side, HALF, HALF), 3, dp=q.right,
        )
        self.c_sb = self.start(
            self.chunk(self.total, q.before * PLANE, HALF),
            self.chunk(self.side, PLANE, HALF), 4, dp=q.left,
        )

    def relay(self):
        q = self.place
        for copy, place, slot_from, slot, target, side in (
            (self.c_na, q.after * PLANE, 0, 5, q.right, 0),
            (self.c_nb, q.before * PLANE + HALF, HALF, 6, q.left, PLANE + HALF),
        ):
            copy.wait_recv()

            @pl.loop(0, HALF)
            def _(i, place=place, slot_from=slot_from):
                rows = pl.ds(place + i, 1)
                self.total[:, rows] = (
                    self.total[:, rows].astype(jnp.float32)
                    + self.near[:, pl.ds(slot_from + i, 1)].astype(jnp.float32)
                ).astype(self.dtype)

            c = self.start(
                self.chunk(self.total, place, HALF), self.chunk(self.side, side, HALF), slot, dp=target
            )
            if slot == 5:
                self.c_ra = c
            else:
                self.c_rb = c

    def spread(self):
        q = self.place
        for c in (self.c_sa, self.c_sb, self.c_ra, self.c_rb):
            c.wait_recv()

        @pl.loop(0, PLANE)
        def _(i):
            self.part[:, pl.ds(i, 1)] = (
                self.total[:, pl.ds(q.k * PLANE + i, 1)].astype(jnp.float32)
                + self.side[:, pl.ds(i, 1)].astype(jnp.float32)
                + self.side[:, pl.ds(PLANE + i, 1)].astype(jnp.float32)
            ).astype(self.dtype)

        @pl.loop(1, PLANE)
        def _(j):
            p = lax.rem(q.p + j, PLANE)
            self.copy(
                self.chunk(self.part, p, 1), self.chunk(self.fan, j - 1, 1), 7,
                (q.peer(p), q.core),
            ).start()

    def wait_fan(self, slot, ref, recv):
        s, r = self.sems(slot)
        fifteen = self.chunk(ref, 0, PLANE - 1)
        pltpu.make_async_copy(fifteen, fifteen, r if recv else s).wait()

    def finish(self):
        q = self.place
        self.wait_fan(7, self.fan, True)
        acc = self.part[:, pl.ds(q.p, 1)].astype(jnp.float32)
        for i in range(PLANE - 1):
            acc = acc + self.fan[:, pl.ds(i, 1)].astype(jnp.float32)
        acc = acc.astype(self.dtype)
        self.final[...] = acc
        here = q.k * PLANE + q.p
        self.out[:, pl.ds(here, 1)] = acc

        @pl.loop(1, PLANE)
        def _(j):
            p = lax.rem(q.p + j, PLANE)
            self.copy(
                self.final, self.chunk(self.out, here, 1), 8, (q.peer(p), q.core)
            ).start()

    def share(self):
        q = self.place
        self.wait_fan(8, self.out, True)
        low = self.chunk(self.out, q.k * PLANE, HALF)
        high = self.chunk(self.out, q.k * PLANE + HALF, HALF)
        self.c_gl = self.start(low, low, 9, dp=q.right)
        self.c_gh = self.start(high, high, 10, dp=q.left)
        self.c_hh = self.start(high, high, 11, dp=q.right)
        self.c_hl = self.start(low, low, 12, dp=q.left)

    def forward(self):
        q = self.place
        self.c_gl.wait_recv()
        low = self.chunk(self.out, q.before * PLANE, HALF)
        self.c_fl = self.start(low, low, 13, dp=q.right)
        self.c_gh.wait_recv()
        high = self.chunk(self.out, q.after * PLANE + HALF, HALF)
        self.c_fh = self.start(high, high, 14, dp=q.left)

    def close(self):
        for c in (self.c_hh, self.c_hl, self.c_fl, self.c_fh):
            c.wait_recv()

    def drain(self):
        for c in self.pending:
            c.wait_send()
        self.wait_fan(7, self.fan, False)
        self.wait_fan(8, self.out, False)


SLOTS = 15


def greet(places):
    barrier = pltpu.get_barrier_semaphore()
    me = lax.axis_index("dp")
    core = places[0].core
    pl.semaphore_signal(barrier, inc=1, device_id=(me, 1 - core), device_id_type=MESH)
    for q in places:
        @pl.loop(1, PLANE)
        def _(j, q=q):
            pl.semaphore_signal(
                barrier, inc=1,
                device_id=(q.peer(lax.rem(q.p + j, PLANE)), core), device_id_type=MESH,
            )
    pl.semaphore_wait(barrier, 1 + 3 * (PLANE - 1))


def reduce_kernel(*args):
    own, other, out = args[0:4], args[4:8], args[8:12]
    rest = args[12:]
    names = ("arrive", "total", "near", "side", "part", "fan", "final")
    refs = {name: rest[4 * i : 4 * i + 4] for i, name in enumerate(names)}
    refs.update(own=own, other=other, out=out)
    refs["send"], refs["recv"] = rest[4 * len(names) :]
    places = [Place(a) for a in range(3)]
    greet(places)
    streams = [Stream(i, refs, places) for i in range(len(STREAMS))]
    for s in streams:
        s.swap()
    for step in ("combine", "relay", "spread", "finish", "share", "forward", "close", "drain"):
        for s in streams:
            getattr(s, step)()


def shapes(count):
    return [
        pltpu.VMEM((BLOCKS[g], count, ROWS[g], 128), TYPES[g]) for g in range(4)
    ]


def reduce_all(own, other):
    vmem = pl.BlockSpec(memory_space=pltpu.VMEM)
    return pl.pallas_call(
        reduce_kernel,
        out_shape=[
            jax.ShapeDtypeStruct((BLOCKS[g], CHUNKS, ROWS[g], 128), TYPES[g]) for g in range(4)
        ],
        in_specs=[vmem] * 8,
        out_specs=[vmem] * 4,
        scratch_shapes=(
            shapes(CHUNKS)
            + shapes(CHUNKS)
            + shapes(PLANE)
            + shapes(2 * PLANE)
            + shapes(PLANE)
            + shapes(PLANE - 1)
            + shapes(1)
            + [
                pltpu.SemaphoreType.DMA((len(STREAMS), SLOTS)),
                pltpu.SemaphoreType.DMA((len(STREAMS), SLOTS)),
            ]
        ),
        compiler_params=pltpu.CompilerParams(
            collective_id=0, has_side_effects=True, vmem_limit_bytes=60 * 1024 * 1024
        ),
        name="reduce_all",
    )(*own, *other)


def features_of(ids, hash_mult, hash_add):
    hashed = jnp.remainder(ids[:, None] * hash_mult[None, :] + hash_add[None, :], modulus)
    return (hashed.astype(jnp.float32) * (2.0 / 1000002.0) - 1.0).astype(jnp.bfloat16)


def silu_grad(value):
    sig = jax.nn.sigmoid(value)
    return sig * (1.0 + value * (1.0 - sig))


def from_everyone(array, axis):
    size = lax.axis_size(axis)
    return lax.all_to_all(
        jnp.broadcast_to(array[None], (size, *array.shape)), axis, 0, 0, tiled=True
    )


def in_order(tiles, dim):
    dims = list(tiles.shape[1:])
    dims[dim] *= tiles.shape[0]
    return jnp.moveaxis(tiles, 0, dim).reshape(dims)


def gather_directly(array, axis, dim):
    return in_order(from_everyone(array, axis), dim)


def tall(g):
    return g.reshape(CHUNKS, 16, 4, 128).transpose(2, 0, 1, 3).astype(jnp.bfloat16)


def from_tall(t):
    return t.astype(jnp.float32).transpose(1, 2, 0, 3).reshape(1024, 512)


def wide(g):
    return g.reshape(512, 4, 2, 128).transpose(1, 2, 0, 3).reshape(4, CHUNKS, 16, 128).astype(jnp.bfloat16)


def from_wide(t):
    return t.astype(jnp.float32).reshape(4, 2, 512, 128).transpose(2, 0, 1, 3).reshape(512, 1024)


def local(
    hot_rows, hot_count, hot_cot, table, cold_ids, hash_mult, hash_add,
    layer_one, layer_two, layer_three, layer_four, cold_cot,
):
    width = table.shape[1]
    core = lax.axis_index("mp")
    span = hot_rows.shape[2] // 2
    begin = core * span
    f32 = jnp.float32

    def dot(a, b):
        return jnp.dot(a, b, preferred_element_type=f32)

    def partner(x):
        return lax.ppermute(x, "mp", [(0, 1), (1, 0)])

    w1, w2, w3, w4 = layer_one, layer_two, layer_three, layer_four
    v1, v2, v3, v4 = partner(w1), partner(w2), partner(w3), partner(w4)
    tokens = cold_ids.shape[0] // 2
    ids = lax.dynamic_slice_in_dim(cold_ids, core * tokens, tokens, 0)
    cot = lax.dynamic_slice_in_dim(cold_cot, core * tokens, tokens, 0)
    feats = features_of(ids, hash_mult, hash_add)

    def act(v):
        return jax.nn.silu(v).astype(jnp.bfloat16)

    p1, q1 = dot(feats, w1), dot(feats, v1)
    a1, c1 = act(p1), act(q1)
    p2 = dot(a1, w2) + dot(c1, v2)
    a2 = act(p2)
    p3, q3 = dot(a2, w3), dot(a2, v3)
    a3, c3 = act(p3), act(q3)
    emb = (dot(a3, w4) + dot(c3, v4)).astype(jnp.bfloat16)
    emb_other = partner(emb)
    first = jnp.where(core == 0, emb, emb_other)
    last = jnp.where(core == 0, emb_other, emb)
    cold_emb = jnp.concatenate([first, last], 0)

    def back(v, pre):
        return (v * silu_grad(pre)).astype(jnp.bfloat16)

    b3, d3 = back(dot(cot, w4.T), p3), back(dot(cot, v4.T), q3)
    g4, h4 = dot(a3.T, cot), dot(c3.T, cot)
    b2 = back(dot(b3, w3.T) + dot(d3, v3.T), p2)
    g3, h3 = dot(a2.T, b3), dot(a2.T, d3)
    b1, d1 = back(dot(b2, w2.T), p1), back(dot(b2, v2.T), q1)
    g2, h2 = dot(a1.T, b2), dot(c1.T, b2)
    g1, h1 = dot(feats.T, b1), dot(feats.T, d1)

    own = [tall(g3), g4.reshape(1, CHUNKS, 8, 128), wide(g2), tall(g1)]
    other = [tall(h3), h4.reshape(1, CHUNKS, 8, 128), wide(h2), tall(h1)]
    o3, o4, o2, o1 = reduce_all(own, other)
    factor = float(cold_ids.shape[0] * lax.axis_size("dp")) ** (-0.5)
    grad_one = from_tall(o1) * factor
    grad_two = from_wide(o2) * factor
    grad_three = from_tall(o3) * factor
    grad_four = o4.reshape(512, 128) * factor

    mine = lax.dynamic_slice_in_dim(hot_rows, begin, span, 2)
    received = lax.all_to_all(mine, "dp", split_axis=1, concat_axis=1, tiled=True)
    fetched = jnp.take(table, received.reshape(-1), axis=0).astype(jnp.bfloat16)
    fetched = fetched.reshape(received.shape + (width,))
    returned = lax.all_to_all(fetched, "dp", split_axis=1, concat_axis=1, tiled=True)
    slot_index = begin + jnp.arange(span, dtype=jnp.int32)
    used = slot_index[None, None, :] < hot_count[:, :, None]
    own_emb = jnp.where(used[..., None], returned, jnp.zeros_like(returned))
    own_cot = lax.dynamic_slice_in_dim(hot_cot, begin, span, 2)
    own_cot = jnp.where(used[..., None], own_cot, jnp.zeros_like(own_cot))
    arrived = lax.all_to_all(own_cot, "dp", split_axis=1, concat_axis=1, tiled=True)
    arrived = gather_directly(arrived, "mp", 2)
    received = gather_directly(received, "mp", 2)
    hot_emb = gather_directly(own_emb, "mp", 2)
    delta = (
        jnp.zeros_like(table)
        .at[received.reshape(-1)]
        .add(arrived.reshape(-1, width).astype(jnp.float32))
    )
    new_table = table - learn_rate * delta
    return (hot_emb, new_table, cold_emb, grad_one, grad_two, grad_three, grad_four)


def solution(mesh):
    in_specs = (
        P("dp", None, None),
        P("dp", None),
        P("dp", None, None, None),
        P("dp", None),
        P("dp"),
        P(),
        P(),
        P(None, "mp"),
        P("mp", None),
        P(None, "mp"),
        P("mp", None),
        P("dp", None),
    )
    out_specs = (
        P("dp", None, None, None),
        P("dp", None),
        P("dp", None),
        P(None, "mp"),
        P("mp", None),
        P(None, "mp"),
        P("mp", None),
    )
    return jax.shard_map(local, mesh=mesh, in_specs=in_specs, out_specs=out_specs, check_vma=False)
```

```python
import jax
import jax.numpy as jnp
from jax import lax
from jax.experimental import pallas as pl
from jax.experimental.pallas import tpu as pltpu
from jax.sharding import PartitionSpec as P

MESH = pl.DeviceIdType.MESH
bf16, f32, i32 = jnp.bfloat16, jnp.float32, jnp.int32
learn_rate = 0.5
modulus = 1000003
RING = 4
PLANE = RING * RING
CHUNKS = RING * PLANE
HALF = PLANE // 2
TOKENS = 512
HIDDEN = 1024
MINE = 512
WIDTH = 128
OWNED = 4096
SPAN = 16
ASKED = CHUNKS * SPAN
ROWBLOCK = 512

THREE, FOUR, TWO, ONE = range(4)
LANES = (512, 128, 512, 512)
ROWS = (16, 8, 16, 16)
TYPES = (bf16, f32, bf16, bf16)
STREAMS = (
    (THREE, 0, 2, 0),
    (THREE, 2, 1, 1),
    (THREE, 3, 1, 2),
    (FOUR, 0, 1, 1),
    (TWO, 0, 2, 1),
    (TWO, 2, 1, 2),
    (TWO, 3, 1, 0),
    (ONE, 0, 2, 2),
    (ONE, 2, 1, 0),
    (ONE, 3, 1, 1),
)
SLOTS = 15


class Place:
    def __init__(self, axis):
        me = lax.axis_index("dp")
        self.core = lax.axis_index("mp")
        strides = (1, RING, RING * RING)
        self.stride = strides[axis]
        self.others = (strides[(axis + 1) % 3], strides[(axis + 2) % 3])
        self.k = lax.rem(me // self.stride, RING)
        self.first = lax.rem(me // self.others[0], RING)
        self.second = lax.rem(me // self.others[1], RING)
        self.p = self.first * RING + self.second
        self.after = lax.rem(self.k + 1, RING)
        self.before = lax.rem(self.k + RING - 1, RING)
        self.opposite = lax.rem(self.k + 2, RING)
        self.right = me + (self.after - self.k) * self.stride
        self.left = me + (self.before - self.k) * self.stride

    def peer(self, p):
        return (
            self.k * self.stride
            + (p // RING) * self.others[0]
            + lax.rem(p, RING) * self.others[1]
        )


class Stream:
    def __init__(self, index, refs, places):
        self.grad, b0, nb, axis = STREAMS[index]
        self.place = places[axis]
        self.index = index
        self.lanes = pl.ds(b0 * WIDTH, nb * WIDTH)
        self.lane0, self.nlanes = b0 * WIDTH, nb * WIDTH
        g = self.grad
        for name in ("own", "other", "arrive", "total", "out", "near", "side", "part", "fan", "final"):
            setattr(self, name, refs[name][g])
        self.result = refs["result"][g]
        self.send, self.recv = refs["send"], refs["recv"]
        self.leave = refs["leave"]
        self.dtype = TYPES[g]
        self.pending = []

    def view(self, ref, first, count):
        return ref.at[pl.ds(first, count), :, self.lanes]

    def outview(self, ref, first, count):
        if self.grad != TWO:
            return self.view(ref, first, count)
        half = CHUNKS // 2
        lane = pl.multiple_of((first // half) * 512 + self.lane0, WIDTH)
        return ref.at[pl.ds(lax.rem(first, half), count), :, pl.ds(lane, self.nlanes)]

    def load(self, ref, first, count):
        return ref[pl.ds(first, count), :, self.lanes].astype(f32)

    def store(self, ref, first, count, value):
        ref[pl.ds(first, count), :, self.lanes] = value.astype(self.dtype)

    def copy(self, src, dst, slot, device):
        return pltpu.make_async_remote_copy(
            src_ref=src, dst_ref=dst,
            send_sem=self.send.at[self.index, slot], recv_sem=self.recv.at[self.index, slot],
            device_id=device, device_id_type=MESH,
        )

    def start(self, src, dst, slot, dp=None, mp=None):
        where = (
            lax.axis_index("dp") if dp is None else dp,
            self.place.core if mp is None else mp,
        )
        c = self.copy(src, dst, slot, where)
        c.start()
        self.pending.append(c)
        return c

    def swap(self):
        self.c_swap = self.start(
            self.view(self.other, 0, CHUNKS), self.view(self.arrive, 0, CHUNKS), 0,
            mp=1 - self.place.core,
        )

    def combine(self):
        self.c_swap.wait_recv()

        @pl.loop(0, CHUNKS // 8)
        def _(i):
            self.store(
                self.total, i * 8, 8,
                self.load(self.own, i * 8, 8) + self.load(self.arrive, i * 8, 8),
            )

        q = self.place
        base = q.opposite * PLANE
        self.c_na = self.start(
            self.view(self.total, base, HALF), self.view(self.near, 0, HALF), 1, dp=q.right
        )
        self.c_nb = self.start(
            self.view(self.total, base + HALF, HALF), self.view(self.near, HALF, HALF), 2, dp=q.left
        )
        self.c_sa = self.start(
            self.view(self.total, q.after * PLANE + HALF, HALF),
            self.view(self.side, HALF, HALF), 3, dp=q.right,
        )
        self.c_sb = self.start(
            self.view(self.total, q.before * PLANE, HALF),
            self.view(self.side, PLANE, HALF), 4, dp=q.left,
        )

    def relay(self):
        q = self.place
        low, high = q.after * PLANE, q.before * PLANE + HALF
        self.c_na.wait_recv()
        self.store(
            self.total, low, HALF, self.load(self.total, low, HALF) + self.load(self.near, 0, HALF)
        )
        self.c_ra = self.start(
            self.view(self.total, low, HALF), self.view(self.side, 0, HALF), 5, dp=q.right
        )
        self.c_nb.wait_recv()
        self.store(
            self.total, high, HALF,
            self.load(self.total, high, HALF) + self.load(self.near, HALF, HALF),
        )
        self.c_rb = self.start(
            self.view(self.total, high, HALF), self.view(self.side, PLANE + HALF, HALF), 6, dp=q.left
        )

    def spread(self):
        q = self.place
        for c in (self.c_sa, self.c_sb, self.c_ra, self.c_rb):
            c.wait_recv()

        @pl.loop(0, PLANE // 4)
        def _(i):
            self.store(
                self.part, i * 4, 4,
                self.load(self.total, q.k * PLANE + i * 4, 4)
                + self.load(self.side, i * 4, 4)
                + self.load(self.side, PLANE + i * 4, 4),
            )

        @pl.loop(1, PLANE)
        def _(j):
            p = lax.rem(q.p + j, PLANE)
            self.copy(
                self.view(self.part, p, 1), self.view(self.fan, j - 1, 1), 7, (q.peer(p), q.core)
            ).start()

    def wait_fan(self, slot, recv):
        fifteen = self.view(self.fan, 0, PLANE - 1)
        sem = (self.recv if recv else self.send).at[self.index, slot]
        pltpu.make_async_copy(fifteen, fifteen, sem).wait()

    def finish(self):
        q = self.place
        self.wait_fan(7, True)
        acc = self.load(self.part, q.p, 1)
        for i in range(PLANE - 1):
            acc = acc + self.load(self.fan, i, 1)
        self.store(self.final, 0, 1, acc)
        here = q.k * PLANE + q.p
        self.outview(self.out, here, 1)[...] = acc.astype(self.dtype)

        @pl.loop(1, PLANE)
        def _(j):
            p = lax.rem(q.p + j, PLANE)
            self.copy(
                self.view(self.final, 0, 1), self.outview(self.out, here, 1), 8, (q.peer(p), q.core)
            ).start()

    def share(self):
        q = self.place
        self.wait_fan(8, True)
        low = self.outview(self.out, q.k * PLANE, HALF)
        high = self.outview(self.out, q.k * PLANE + HALF, HALF)
        self.c_gl = self.start(low, low, 9, dp=q.right)
        self.c_gh = self.start(high, high, 10, dp=q.left)
        self.c_hh = self.start(high, high, 11, dp=q.right)
        self.c_hl = self.start(low, low, 12, dp=q.left)

    def forward(self):
        q = self.place
        self.c_gl.wait_recv()
        low = self.outview(self.out, q.before * PLANE, HALF)
        self.c_fl = self.start(low, low, 13, dp=q.right)
        self.c_gh.wait_recv()
        high = self.outview(self.out, q.after * PLANE + HALF, HALF)
        self.c_fh = self.start(high, high, 14, dp=q.left)

    def close(self):
        for c in (self.c_hh, self.c_hl, self.c_fl, self.c_fh):
            c.wait_recv()
        if self.grad == TWO:
            ends = [(0, self.lane0), (0, 512 + self.lane0)]
            count = CHUNKS // 2
        else:
            ends, count = [(0, self.lane0)], CHUNKS
        self.leaving = []
        for n, (first, lane) in enumerate(ends):
            where = (pl.ds(first, count), slice(None), pl.ds(lane, self.nlanes))
            c = pltpu.make_async_copy(
                self.out.at[where], self.result.at[where], self.leave.at[self.index, n]
            )
            c.start()
            self.leaving.append(c)

    def drain(self):
        for c in self.pending:
            c.wait_send()
        self.wait_fan(7, False)
        self.wait_fan(8, False)
        for c in self.leaving:
            c.wait()


class Group:
    def __init__(self, streams):
        self.streams = streams

    def __getattr__(self, step):
        def run():
            for s in self.streams:
                getattr(s, step)()
        return run


def rows_by_columns(a, b):
    return lax.dot_general(a, b, (((0,), (0,)), ((), ())), preferred_element_type=f32)


def times_transposed(a, b):
    return lax.dot_general(a, b, (((1,), (1,)), ((), ())), preferred_element_type=f32)


def tile(n, size=256):
    return pl.ds(pl.multiple_of(n * size, size), size)


def step_kernel(
    asked, ids, mult, add, w1, w2, w3, w4, ccot, hcot, table,
    r3, r4, r2, r1, hot_out, table_out, emb_out,
    *rest,
):
    names = ("own", "other", "arrive", "total", "near", "side", "part", "fan", "final", "out")
    refs = {name: rest[4 * i : 4 * i + 4] for i, name in enumerate(names)}
    rest = rest[4 * len(names) :]
    (
        refs["send"], refs["recv"], refs["leave"],
        w1c, w2c, w3c, w4c, feats, a1, a2, a3, ds1, ds2, ds3, b1, b2, b3, cot, emb,
        tab, tabt, newtab, rowmsg, rowbuf, rowsum, hc, carr, onehot, embt, ebuf, hout,
        loads, wsend, wrecv, hsend, hrecv, stores,
    ) = rest
    refs["result"] = (r3, r4, r2, r1)
    me = lax.axis_index("dp")
    core = lax.axis_index("mp")
    partner = (me, 1 - core)
    places = [Place(a) for a in range(3)]
    streams = [Stream(i, refs, places) for i in range(len(STREAMS))]
    first, second, third = Group(streams[:4]), Group(streams[4:7]), Group(streams[7:])

    load = {}
    for n, (name, src, dst) in enumerate((
        ("w1", w1, w1c.at[:, pl.ds(0, MINE)]),
        ("w2", w2, w2c.at[pl.ds(0, MINE)]),
        ("w3", w3, w3c.at[:, pl.ds(0, MINE)]),
        ("w4", w4, w4c.at[pl.ds(0, MINE)]),
        ("hcot", hcot.at[0, :, pl.ds(pl.multiple_of(core * SPAN, SPAN), SPAN)], hc),
        ("cot", ccot.at[pl.ds(pl.multiple_of(core * TOKENS, TOKENS), TOKENS)], cot),
        ("table", table, tab),
    )):
        load[name] = pltpu.make_async_copy(src, dst, loads.at[n])
        load[name].start()

    barrier = pltpu.get_barrier_semaphore()
    pl.semaphore_signal(barrier, inc=1, device_id=partner, device_id_type=MESH)

    @pl.loop(1, CHUNKS)
    def _(j):
        pl.semaphore_signal(
            barrier, inc=1, device_id=(lax.rem(me + j, CHUNKS), core), device_id_type=MESH
        )

    lane = lax.broadcasted_iota(i32, (CHUNKS, WIDTH), 1)
    begin = core * SPAN
    want = jnp.where((lane >= begin) & (lane < begin + SPAN), asked[...], 0)
    shift = lax.rem(lax.rem(me, 8) * SPAN - begin + WIDTH, WIDTH)
    want = pltpu.roll(want, shift, 1)
    rowmsg[...] = jnp.broadcast_to(want[:, None, :], (CHUNKS, 8, WIDTH))

    for b in range(TOKENS // WIDTH):
        line = ids[pl.ds(core * (TOKENS // WIDTH) + b, 1), :]
        column = jnp.transpose(jnp.broadcast_to(line, (WIDTH, WIDTH)))

        @pl.loop(0, HIDDEN // WIDTH)
        def _(j, b=b, column=column):
            h = column * mult[pl.ds(j, 1), :] + add[pl.ds(j, 1), :]
            q = (h.astype(f32) * (1.0 / modulus)).astype(i32)
            r = h - q * modulus
            r = jnp.where(r < 0, r + modulus, r)
            r = jnp.where(r >= modulus, r - modulus, r)
            feats[pl.ds(b * WIDTH, WIDTH), tile(j, WIDTH)] = (
                r.astype(f32) * (2.0 / 1000002.0) - 1.0
            ).astype(bf16)

    pl.semaphore_wait(barrier, CHUNKS)

    sent = []

    def give(src, dst, n, device):
        c = pltpu.make_async_remote_copy(
            src_ref=src, dst_ref=dst, send_sem=wsend.at[n], recv_sem=wrecv.at[n],
            device_id=device, device_id_type=MESH,
        )
        c.start()
        sent.append(c)
        return c

    mine, theirs = pl.ds(0, MINE), pl.ds(MINE, MINE)
    load["w1"].wait()
    got1 = give(w1c.at[:, mine], w1c.at[:, theirs], 0, partner)
    load["w2"].wait()
    got2 = give(w2c.at[mine], w2c.at[theirs], 1, partner)
    load["w3"].wait()
    got3 = give(w3c.at[:, mine], w3c.at[:, theirs], 2, partner)
    load["w4"].wait()
    got4 = give(w4c.at[mine], w4c.at[theirs], 3, partner)

    load["hcot"].wait()

    def hot(src, dst, n, s):
        return pltpu.make_async_remote_copy(
            src_ref=src, dst_ref=dst, send_sem=hsend.at[n], recv_sem=hrecv.at[n],
            device_id=(s, core), device_id_type=MESH,
        )

    @pl.loop(1, CHUNKS)
    def _(j):
        o = lax.rem(me + j, CHUNKS)
        hot(rowmsg.at[o], rowbuf.at[me], 0, o).start()
        hot(hc.at[o], carr.at[0, me], 1, o).start()

    rowbuf[pl.ds(me, 1)] = rowmsg[pl.ds(me, 1)]
    carr[0, pl.ds(me, 1)] = hc[pl.ds(me, 1)]

    def hot_wait(ref, n, recv):
        sem = (hrecv if recv else hsend).at[n]
        part = ref.at[pl.ds(0, CHUNKS - 1)]
        pltpu.make_async_copy(part, part, sem).wait()

    def activate(pre, act, ds, columns):
        sig = 0.5 * jnp.tanh(0.5 * pre) + 0.5
        act[:, columns] = (pre * sig).astype(bf16)
        ds[:, columns] = sig * (1.0 + pre * (1.0 - sig))

    def layer(src, w, act, ds, lo, hi):
        @pl.loop(lo, hi)
        def _(n):
            pre = jnp.dot(src[...], w[:, tile(n)], preferred_element_type=f32)
            activate(pre, act, ds, tile(n))

    layer(feats, w1c, a1, ds1, 0, 2)
    got1.wait_recv()
    layer(feats, w1c, a1, ds1, 2, 4)
    got2.wait_recv()
    layer(a1, w2c, a2, ds2, 0, 4)
    layer(a2, w3c, a3, ds3, 0, 2)
    got3.wait_recv()
    layer(a2, w3c, a3, ds3, 2, 4)
    got4.wait_recv()
    load["cot"].wait()

    @pl.loop(0, 4)
    def _(n):
        b3[:, tile(n)] = (times_transposed(cot[...], w4c[tile(n), :]) * ds3[:, tile(n)]).astype(bf16)

    def tall_grad(act, back, g, half, ref):
        @pl.loop(0, 4)
        def _(m):
            t = rows_by_columns(act[:, tile(m)], back[:, pl.ds(half * MINE, MINE)])
            ref[g][pl.ds(m * 16, 16)] = t.reshape(16, 16, 512).astype(ref[g].dtype)

    def wide_grad(half, ref):
        @pl.loop(0, 2)
        def _(m):
            for h in range(2):
                t = rows_by_columns(a1[:, tile(m + 2 * half)], b2[:, pl.ds(h * 512, 512)])
                ref[TWO][pl.ds(h * 32 + m * 16, 16)] = t.reshape(16, 16, 512).astype(ref[TWO].dtype)

    def grad_four(half, ref):
        t = rows_by_columns(a3[:, pl.ds(half * MINE, MINE)], cot[...])
        ref[FOUR][...] = t.reshape(CHUNKS, 8, WIDTH)

    own, other = refs["own"], refs["other"]
    tall_grad(a2, b3, THREE, 1, other)
    grad_four(1, other)
    first.swap()
    tall_grad(a2, b3, THREE, 0, own)
    grad_four(0, own)
    first.combine()

    @pl.loop(0, 4)
    def _(n):
        b2[:, tile(n)] = (times_transposed(b3[...], w3c[tile(n), :]) * ds2[:, tile(n)]).astype(bf16)

    wide_grad(1, other)
    second.swap()
    first.relay()
    wide_grad(0, own)
    second.combine()

    @pl.loop(0, 4)
    def _(n):
        b1[:, tile(n)] = (times_transposed(b2[...], w2c[tile(n), :]) * ds1[:, tile(n)]).astype(bf16)

    tall_grad(feats, b1, ONE, 1, other)
    third.swap()
    first.spread()
    second.relay()
    tall_grad(feats, b1, ONE, 0, own)
    third.combine()

    emb[core] = jnp.dot(a3[...], w4c[...], preferred_element_type=f32).astype(bf16)
    got_emb = give(emb.at[core], emb.at[core], 4, partner)

    hot_wait(rowbuf, 0, True)
    for g in range(8):
        total = rowbuf[8 * g]
        for i in range(1, 8):
            total = total + rowbuf[8 * g + i]
        rowsum[0, g] = total
    got_rows = give(rowsum.at[0], rowsum.at[1], 5, partner)
    hot_wait(carr.at[0], 1, True)
    got_carr = give(carr.at[0], carr.at[1], 6, partner)
    first.finish()
    load["table"].wait()

    @pl.loop(0, OWNED // WIDTH)
    def _(n):
        tabt[:, tile(n, WIDTH)] = jnp.transpose(tab[tile(n, WIDTH), :]).astype(bf16)

    def select(which, block):
        row = lax.broadcasted_iota(i32, (ROWBLOCK, WIDTH), 0) + (block * ROWBLOCK + 1)
        for g in range(8):
            hit = row == jnp.broadcast_to(rowsum[which, g][0:1, :], (ROWBLOCK, WIDTH))
            onehot[:, pl.ds(g * WIDTH, WIDTH)] = jnp.where(hit, 1.0, 0.0).astype(bf16)

    second.spread()
    third.relay()
    embt[...] = jnp.zeros_like(embt)

    @pl.loop(0, OWNED // ROWBLOCK)
    def _(n):
        select(0, n)
        embt[...] += jnp.dot(tabt[:, tile(n, ROWBLOCK)], onehot[...], preferred_element_type=f32)

    for g in range(8):
        found = jnp.transpose(embt[:, pl.ds(g * WIDTH, WIDTH)]).astype(bf16)
        ebuf[pl.ds(g * 8, 8)] = found.reshape(8, SPAN, WIDTH)

    @pl.loop(1, CHUNKS)
    def _(j):
        s = lax.rem(me + j, CHUNKS)
        hot(ebuf.at[s], hout.at[me, core], 2, s).start()

    hout[pl.ds(me, 1), pl.ds(core, 1)] = ebuf[pl.ds(me, 1)][:, None]

    first.share()
    second.finish()
    third.spread()
    got_rows.wait_recv()
    got_carr.wait_recv()

    def update(lo, hi):
        @pl.loop(lo, hi)
        def _(n):
            rows = tile(n, ROWBLOCK)
            select(0, n)
            delta = jnp.dot(onehot[...], carr[0].reshape(ASKED, WIDTH), preferred_element_type=f32)
            select(1, n)
            delta += jnp.dot(onehot[...], carr[1].reshape(ASKED, WIDTH), preferred_element_type=f32)
            newtab[rows, :] = tab[rows, :] - learn_rate * delta

    update(0, 2)
    first.forward()
    second.share()
    third.finish()
    update(2, 4)
    first.close()
    second.forward()
    third.share()
    update(4, 6)
    third.forward()
    hot_wait(hout.at[:, 0], 2, True)
    got_hot = give(hout.at[:, core], hout.at[:, core], 7, partner)
    update(6, 8)
    put_table = pltpu.make_async_copy(newtab, table_out, stores.at[0])
    put_table.start()
    second.close()
    got_emb.wait_recv()
    put_emb = pltpu.make_async_copy(emb, emb_out, stores.at[1])
    put_emb.start()
    got_hot.wait_recv()
    put_hot = pltpu.make_async_copy(hout, hot_out, stores.at[2])
    put_hot.start()
    third.close()

    for group in (first, second, third):
        group.drain()
    for c in sent:
        c.wait_send()
    hot_wait(rowbuf, 0, False)
    hot_wait(carr.at[0], 1, False)
    hot_wait(ebuf, 2, False)
    for c in (put_table, put_emb, put_hot):
        c.wait()


def shapes(count, types=TYPES):
    return [pltpu.VMEM((count, ROWS[g], LANES[g]), types[g]) for g in range(4)]


def outs(kind):
    sizes = [(CHUNKS, ROWS[g], LANES[g]) for g in range(4)]
    sizes[TWO] = (CHUNKS // 2, 16, 1024)
    return [kind(sizes[g], TYPES[g]) for g in range(4)]


def step(*args):
    vmem = pl.BlockSpec(memory_space=pltpu.VMEM)
    anywhere = pl.BlockSpec(memory_space=pl.ANY)
    dma = pltpu.SemaphoreType.DMA
    square = (HIDDEN, HIDDEN)
    tokens = (TOKENS, HIDDEN)
    return pl.pallas_call(
        step_kernel,
        out_shape=outs(jax.ShapeDtypeStruct) + [
            jax.ShapeDtypeStruct((CHUNKS, 2, SPAN, WIDTH), bf16),
            jax.ShapeDtypeStruct((OWNED, WIDTH), f32),
            jax.ShapeDtypeStruct((2, TOKENS, WIDTH), bf16),
        ],
        in_specs=[vmem] * 4 + [anywhere] * 7,
        out_specs=[anywhere] * 7,
        scratch_shapes=(
            shapes(CHUNKS, (f32,) * 4)
            + shapes(CHUNKS)
            + shapes(CHUNKS)
            + shapes(CHUNKS)
            + shapes(PLANE)
            + shapes(2 * PLANE)
            + shapes(PLANE)
            + shapes(PLANE - 1)
            + shapes(1)
            + outs(pltpu.VMEM)
            + [dma((len(STREAMS), SLOTS)), dma((len(STREAMS), SLOTS)), dma((len(STREAMS), 2))]
            + [pltpu.VMEM(square, bf16)] * 3
            + [pltpu.VMEM((HIDDEN, WIDTH), bf16)]
            + [pltpu.VMEM(tokens, bf16)] * 4
            + [pltpu.VMEM(tokens, f32)] * 3
            + [pltpu.VMEM(tokens, bf16)] * 3
            + [
                pltpu.VMEM((TOKENS, WIDTH), bf16),
                pltpu.VMEM((2, TOKENS, WIDTH), bf16),
                pltpu.VMEM((OWNED, WIDTH), f32),
                pltpu.VMEM((WIDTH, OWNED), bf16),
                pltpu.VMEM((OWNED, WIDTH), f32),
                pltpu.VMEM((CHUNKS, 8, WIDTH), i32),
                pltpu.VMEM((CHUNKS, 8, WIDTH), i32),
                pltpu.VMEM((2, 8, 8, WIDTH), i32),
                pltpu.VMEM((CHUNKS, SPAN, WIDTH), bf16),
                pltpu.VMEM((2, CHUNKS, SPAN, WIDTH), bf16),
                pltpu.VMEM((ROWBLOCK, ASKED), bf16),
                pltpu.VMEM((WIDTH, ASKED), f32),
                pltpu.VMEM((CHUNKS, SPAN, WIDTH), bf16),
                pltpu.VMEM((CHUNKS, 2, SPAN, WIDTH), bf16),
                dma((7,)), dma((8,)), dma((8,)), dma((3,)), dma((3,)), dma((3,)),
            ]
        ),
        compiler_params=pltpu.CompilerParams(
            collective_id=0, has_side_effects=True, vmem_limit_bytes=67043328
        ),
        name="step",
    )(*args)


def local(
    hot_rows, hot_count, hot_cot, table, cold_ids, hash_mult, hash_add,
    layer_one, layer_two, layer_three, layer_four, cold_cot,
):
    slots = jnp.arange(hot_rows.shape[2], dtype=i32)
    asked = jnp.where(slots[None, :] < hot_count[0][:, None], hot_rows[0] + 1, 0)
    asked = jnp.pad(asked, ((0, 0), (0, WIDTH - asked.shape[1])))
    r3, r4, r2, r1, hot_emb, new_table, cold_emb = step(
        asked, cold_ids.reshape(8, WIDTH), hash_mult.reshape(8, WIDTH), hash_add.reshape(8, WIDTH),
        layer_one, layer_two, layer_three, layer_four, cold_cot, hot_cot, table,
    )
    factor = float(cold_ids.shape[0] * lax.axis_size("dp")) ** (-0.5)
    return (
        hot_emb.reshape(hot_cot.shape),
        new_table,
        cold_emb.reshape(cold_cot.shape),
        r1.reshape(layer_one.shape).astype(f32) * factor,
        r2.reshape(layer_two.shape).astype(f32) * factor,
        r3.reshape(layer_three.shape).astype(f32) * factor,
        r4.reshape(layer_four.shape) * factor,
    )


def solution(mesh):
    in_specs = (
        P("dp", None, None),
        P("dp", None),
        P("dp", None, None, None),
        P("dp", None),
        P("dp"),
        P(),
        P(),
        P(None, "mp"),
        P("mp", None),
        P(None, "mp"),
        P("mp", None),
        P("dp", None),
    )
    out_specs = (
        P("dp", None, None, None),
        P("dp", None),
        P("dp", None),
        P(None, "mp"),
        P("mp", None),
        P(None, "mp"),
        P("mp", None),
    )
    return jax.shard_map(local, mesh=mesh, in_specs=in_specs, out_specs=out_specs, check_vma=False)
```

```python
import jax
import jax.numpy as jnp
from jax import lax
from jax.experimental import pallas as pl
from jax.experimental.pallas import tpu as pltpu
from jax.sharding import PartitionSpec as P

MESH = pl.DeviceIdType.MESH
bf16, f32, i32 = jnp.bfloat16, jnp.float32, jnp.int32
learn_rate = 0.5
modulus = 1000003
RING = 4
PLANE = RING * RING
CHUNKS = RING * PLANE
HALF = PLANE // 2
TOKENS = 512
HIDDEN = 1024
MINE = 512
WIDTH = 128
OWNED = 4096
SPAN = 16
ASKED = CHUNKS * SPAN
ROWBLOCK = 512

THREE, FOUR, TWO, ONE = range(4)
LANES = (512, 128, 512, 512)
ROWS = (16, 8, 16, 16)
TYPES = (bf16, f32, bf16, bf16)
STREAMS = (
    (THREE, 0, 2, 0),
    (THREE, 2, 1, 1),
    (THREE, 3, 1, 2),
    (FOUR, 0, 1, 1),
    (TWO, 0, 2, 1),
    (TWO, 2, 1, 2),
    (TWO, 3, 1, 0),
    (ONE, 0, 2, 2),
    (ONE, 2, 1, 0),
    (ONE, 3, 1, 1),
)
SLOTS = 15


class Place:
    def __init__(self, axis):
        me = lax.axis_index("dp")
        self.core = lax.axis_index("mp")
        strides = (1, RING, RING * RING)
        self.stride = strides[axis]
        self.others = (strides[(axis + 1) % 3], strides[(axis + 2) % 3])
        self.k = lax.rem(lax.div(me, self.stride), RING)
        self.first = lax.rem(lax.div(me, self.others[0]), RING)
        self.second = lax.rem(lax.div(me, self.others[1]), RING)
        self.p = self.first * RING + self.second
        self.after = lax.rem(self.k + 1, RING)
        self.before = lax.rem(self.k + RING - 1, RING)
        self.opposite = lax.rem(self.k + 2, RING)
        self.right = me + (self.after - self.k) * self.stride
        self.left = me + (self.before - self.k) * self.stride

    def peer(self, p):
        return (
            self.k * self.stride
            + lax.div(p, RING) * self.others[0]
            + lax.rem(p, RING) * self.others[1]
        )


class Stream:
    def __init__(self, index, refs, places):
        self.grad, b0, nb, axis = STREAMS[index]
        self.place = places[axis]
        self.index = index
        self.lanes = pl.ds(b0 * WIDTH, nb * WIDTH)
        self.lane0, self.nlanes = b0 * WIDTH, nb * WIDTH
        g = self.grad
        for name in ("own", "other", "arrive", "total", "out", "near", "side", "part", "fan", "final"):
            setattr(self, name, refs[name][g])
        self.send, self.recv = refs["send"], refs["recv"]
        self.dtype = TYPES[g]
        self.pending = []

    def view(self, ref, first, count):
        return ref.at[pl.ds(first, count), :, self.lanes]

    def outview(self, ref, first, count):
        if self.grad != TWO:
            return self.view(ref, first, count)
        half = CHUNKS // 2
        lane = pl.multiple_of(lax.div(first, half) * 512 + self.lane0, WIDTH)
        return ref.at[pl.ds(lax.rem(first, half), count), :, pl.ds(lane, self.nlanes)]

    def load(self, ref, first, count):
        return ref[pl.ds(first, count), :, self.lanes].astype(f32)

    def store(self, ref, first, count, value):
        ref[pl.ds(first, count), :, self.lanes] = value.astype(self.dtype)

    def copy(self, src, dst, slot, device):
        return pltpu.make_async_remote_copy(
            src_ref=src, dst_ref=dst,
            send_sem=self.send.at[self.index, slot], recv_sem=self.recv.at[self.index, slot],
            device_id=device, device_id_type=MESH,
        )

    def start(self, src, dst, slot, dp=None, mp=None):
        where = (
            lax.axis_index("dp") if dp is None else dp,
            self.place.core if mp is None else mp,
        )
        c = self.copy(src, dst, slot, where)
        c.start()
        self.pending.append(c)
        return c

    def swap(self):
        self.c_swap = self.start(
            self.view(self.other, 0, CHUNKS), self.view(self.arrive, 0, CHUNKS), 0,
            mp=1 - self.place.core,
        )

    def combine(self):
        self.c_swap.wait_recv()

        @pl.loop(0, CHUNKS // 8, unroll=2)
        def _(i):
            self.store(
                self.total, i * 8, 8,
                self.load(self.own, i * 8, 8) + self.load(self.arrive, i * 8, 8),
            )

        q = self.place
        base = q.opposite * PLANE
        self.c_na = self.start(
            self.view(self.total, base, HALF), self.view(self.near, 0, HALF), 1, dp=q.right
        )
        self.c_nb = self.start(
            self.view(self.total, base + HALF, HALF), self.view(self.near, HALF, HALF), 2, dp=q.left
        )
        self.c_sa = self.start(
            self.view(self.total, q.after * PLANE + HALF, HALF),
            self.view(self.side, HALF, HALF), 3, dp=q.right,
        )
        self.c_sb = self.start(
            self.view(self.total, q.before * PLANE, HALF),
            self.view(self.side, PLANE, HALF), 4, dp=q.left,
        )

    def relay(self):
        q = self.place
        low, high = q.after * PLANE, q.before * PLANE + HALF
        self.c_na.wait_recv()
        self.store(
            self.total, low, HALF, self.load(self.total, low, HALF) + self.load(self.near, 0, HALF)
        )
        self.c_ra = self.start(
            self.view(self.total, low, HALF), self.view(self.side, 0, HALF), 5, dp=q.right
        )
        self.c_nb.wait_recv()
        self.store(
            self.total, high, HALF,
            self.load(self.total, high, HALF) + self.load(self.near, HALF, HALF),
        )
        self.c_rb = self.start(
            self.view(self.total, high, HALF), self.view(self.side, PLANE + HALF, HALF), 6, dp=q.left
        )

    def spread(self):
        q = self.place
        for c in (self.c_sa, self.c_sb, self.c_ra, self.c_rb):
            c.wait_recv()

        @pl.loop(0, PLANE // 4, unroll=2)
        def _(i):
            self.store(
                self.part, i * 4, 4,
                self.load(self.total, q.k * PLANE + i * 4, 4)
                + self.load(self.side, i * 4, 4)
                + self.load(self.side, PLANE + i * 4, 4),
            )

        @pl.loop(1, PLANE, unroll=5)
        def _(j):
            p = lax.rem(q.p + j, PLANE)
            self.copy(
                self.view(self.part, p, 1), self.view(self.fan, j - 1, 1), 7, (q.peer(p), q.core)
            ).start()

    def wait_fan(self, slot, recv):
        fifteen = self.view(self.fan, 0, PLANE - 1)
        sem = (self.recv if recv else self.send).at[self.index, slot]
        pltpu.make_async_copy(fifteen, fifteen, sem).wait()

    def finish(self):
        q = self.place
        self.wait_fan(7, True)
        acc = self.load(self.part, q.p, 1)
        for i in range(PLANE - 1):
            acc = acc + self.load(self.fan, i, 1)
        self.store(self.final, 0, 1, acc)
        here = q.k * PLANE + q.p
        self.outview(self.out, here, 1)[...] = acc.astype(self.dtype)

        @pl.loop(1, PLANE, unroll=5)
        def _(j):
            p = lax.rem(q.p + j, PLANE)
            self.copy(
                self.view(self.final, 0, 1), self.outview(self.out, here, 1), 8, (q.peer(p), q.core)
            ).start()

    def share(self):
        q = self.place
        self.wait_fan(8, True)
        low = self.outview(self.out, q.k * PLANE, HALF)
        high = self.outview(self.out, q.k * PLANE + HALF, HALF)
        self.c_gl = self.start(low, low, 9, dp=q.right)
        self.c_gh = self.start(high, high, 10, dp=q.left)
        self.c_hh = self.start(high, high, 11, dp=q.right)
        self.c_hl = self.start(low, low, 12, dp=q.left)

    def forward(self):
        q = self.place
        self.c_gl.wait_recv()
        low = self.outview(self.out, q.before * PLANE, HALF)
        self.c_fl = self.start(low, low, 13, dp=q.right)
        self.c_gh.wait_recv()
        high = self.outview(self.out, q.after * PLANE + HALF, HALF)
        self.c_fh = self.start(high, high, 14, dp=q.left)

    def close(self):
        for c in (self.c_hh, self.c_hl, self.c_fl, self.c_fh):
            c.wait_recv()

    def drain(self):
        for c in self.pending:
            c.wait_send()
        self.wait_fan(7, False)
        self.wait_fan(8, False)


class Group:
    def __init__(self, streams):
        self.streams = streams

    def __getattr__(self, step):
        def run():
            for s in self.streams:
                getattr(s, step)()
        return run


def rows_by_columns(a, b):
    return lax.dot_general(a, b, (((0,), (0,)), ((), ())), preferred_element_type=f32)


def times_transposed(a, b):
    return lax.dot_general(a, b, (((1,), (1,)), ((), ())), preferred_element_type=f32)


def tile(n, size=256):
    return pl.ds(pl.multiple_of(n * size, size), size)


def step_kernel(
    rows_in, count_in, ids_in, mult_in, add_in, w1, w2, w3, w4, ccot, hcot, table,
    r3, r4, r2, r1, hout, newtab, emb,
    *rest,
):
    names = ("other", "arrive", "total", "near", "side", "part", "fan", "final")
    refs = {name: rest[4 * i : 4 * i + 4] for i, name in enumerate(names)}
    rest = rest[4 * len(names) :]
    (
        refs["send"], refs["recv"], own_large, own_four,
        w1c, w2c, w3c, w4c, feats, a1, a2, a3, ds1, ds2, ds3, b2, b3, cot,
        tab, tabt, spare, rowmsg, rowbuf, rowsum, hc, carr, onehot, twohot, embt, ebuf,
        loads, wsend, wrecv, hsend, hrecv, rows, count, ids, mult, add,
    ) = rest
    b1 = b3
    refs["out"] = (r3, r4, r2, r1)
    refs["own"] = (own_large, own_four, own_large, own_large)
    me = lax.axis_index("dp")
    core = lax.axis_index("mp")
    partner = (me, 1 - core)
    places = [Place(a) for a in range(3)]
    streams = [Stream(i, refs, places) for i in range(len(STREAMS))]
    first, second, third = Group(streams[:4]), Group(streams[4:7]), Group(streams[7:])

    load = {}
    for n, (name, src, dst) in enumerate((
        ("rows", rows_in, rows),
        ("count", count_in, count),
        ("ids", ids_in, ids),
        ("mult", mult_in, mult),
        ("add", add_in, add),
        ("w1", w1, w1c.at[:, pl.ds(0, MINE)]),
        ("w2", w2, w2c.at[pl.ds(0, MINE)]),
        ("w3", w3, w3c.at[:, pl.ds(0, MINE)]),
        ("w4", w4, w4c.at[pl.ds(0, MINE)]),
        ("hcot", hcot.at[0, :, pl.ds(pl.multiple_of(core * SPAN, SPAN), SPAN)], hc),
        ("cot", ccot.at[pl.ds(pl.multiple_of(core * TOKENS, TOKENS), TOKENS)], cot),
        ("table", table, tab),
    )):
        load[name] = pltpu.make_async_copy(src, dst, loads.at[n])
        load[name].start()

    barrier = pltpu.get_barrier_semaphore()
    pl.semaphore_signal(barrier, inc=1, device_id=partner, device_id_type=MESH)

    @pl.loop(1, CHUNKS, unroll=7)
    def _(j):
        pl.semaphore_signal(
            barrier, inc=1, device_id=(lax.rem(me + j, CHUNKS), core), device_id_type=MESH
        )

    for name in ("rows", "count", "ids", "mult", "add"):
        load[name].wait()
    slot = lax.broadcasted_iota(i32, (SPAN, CHUNKS), 0) + core * SPAN
    want = rows[0, pl.ds(pl.multiple_of(core * SPAN, SPAN), SPAN), :] + 1
    spare[...] = jnp.zeros_like(spare)
    spare[pl.ds(pl.multiple_of(lax.rem(me, 8) * SPAN, SPAN), SPAN), pl.ds(0, CHUNKS)] = jnp.where(
        slot < count[...], want, 0
    )
    want = jnp.transpose(spare[...])[:CHUNKS]
    rowmsg[...] = jnp.broadcast_to(want[:, None, :], (CHUNKS, 8, WIDTH))

    for b in range(TOKENS // WIDTH):
        line = ids[pl.ds(core * (TOKENS // WIDTH) + b, 1), :]
        column = jnp.transpose(jnp.broadcast_to(line, (WIDTH, WIDTH)))

        @pl.loop(0, HIDDEN // WIDTH, unroll=2)
        def _(j, b=b, column=column):
            h = column * mult[pl.ds(j, 1), :] + add[pl.ds(j, 1), :]
            q = (h.astype(f32) * ((1.0 - 4e-7) / modulus)).astype(i32)
            r = h - q * modulus
            r = jnp.where(r >= modulus, r - modulus, r)
            feats[pl.ds(b * WIDTH, WIDTH), tile(j, WIDTH)] = (
                r.astype(f32) * (2.0 / 1000002.0) - 1.0
            ).astype(bf16)

    pl.semaphore_wait(barrier, CHUNKS)

    sent = []

    def give(src, dst, n, device):
        c = pltpu.make_async_remote_copy(
            src_ref=src, dst_ref=dst, send_sem=wsend.at[n], recv_sem=wrecv.at[n],
            device_id=device, device_id_type=MESH,
        )
        c.start()
        sent.append(c)
        return c

    mine, theirs = pl.ds(0, MINE), pl.ds(MINE, MINE)
    load["w1"].wait()
    got1 = [
        give(w1c.at[:, pl.ds(256 * n, 256)], w1c.at[:, pl.ds(MINE + 256 * n, 256)], n, partner)
        for n in range(2)
    ]
    load["w2"].wait()
    got2 = give(w2c.at[mine], w2c.at[theirs], 9, partner)

    load["table"].wait()

    @pl.loop(0, OWNED // WIDTH, unroll=8)
    def _(n):
        tabt[:, tile(n, WIDTH)] = jnp.transpose(tab[tile(n, WIDTH), :]).astype(bf16)

    load["hcot"].wait()

    def hot(src, dst, n, s):
        return pltpu.make_async_remote_copy(
            src_ref=src, dst_ref=dst, send_sem=hsend.at[n], recv_sem=hrecv.at[n],
            device_id=(s, core), device_id_type=MESH,
        )

    @pl.loop(1, CHUNKS, unroll=7)
    def _(j):
        o = lax.rem(me + j, CHUNKS)
        hot(rowmsg.at[o], rowbuf.at[me], 0, o).start()
        hot(hc.at[o], carr.at[0, me], 1, o).start()

    rowbuf[pl.ds(me, 1)] = rowmsg[pl.ds(me, 1)]
    carr[0, pl.ds(me, 1)] = hc[pl.ds(me, 1)]

    def hot_wait(ref, n, recv):
        sem = (hrecv if recv else hsend).at[n]
        part = ref.at[pl.ds(0, CHUNKS - 1)]
        pltpu.make_async_copy(part, part, sem).wait()

    def activate(pre, act, ds, columns):
        sig = 0.5 * jnp.tanh(0.5 * pre) + 0.5
        act[:, columns] = (pre * sig).astype(bf16)
        ds[:, columns] = sig * (1.0 + pre * (1.0 - sig))

    def layer(src, w, act, ds, lo, hi):
        for n in range(lo, hi):
            columns = pl.ds(n * 256, 256)
            pre = jnp.dot(src[...], w[:, columns], preferred_element_type=f32)
            activate(pre, act, ds, columns)

    layer(feats, w1c, a1, ds1, 0, 2)
    load["w3"].wait()
    got3 = give(w3c.at[:, mine], w3c.at[:, theirs], 2, partner)
    load["w4"].wait()
    got4 = give(w4c.at[mine], w4c.at[theirs], 3, partner)
    got1[0].wait_recv()
    layer(feats, w1c, a1, ds1, 2, 3)
    got1[1].wait_recv()
    layer(feats, w1c, a1, ds1, 3, 4)
    got2.wait_recv()
    layer(a1, w2c, a2, ds2, 0, 4)
    layer(a2, w3c, a3, ds3, 0, 2)
    got3.wait_recv()
    layer(a2, w3c, a3, ds3, 2, 4)
    got4.wait_recv()
    load["cot"].wait()

    def backward(src, w, ds, out):
        for n in range(4):
            columns = pl.ds(n * 256, 256)
            out[:, columns] = (times_transposed(src[...], w[columns, :]) * ds[:, columns]).astype(bf16)

    backward(cot, w4c, ds3, b3)

    def tall_grad(act, back, g, half, ref):
        for m in range(4):
            t = rows_by_columns(act[:, pl.ds(m * 256, 256)], back[:, pl.ds(half * MINE, MINE)])
            ref[g][pl.ds(m * 16, 16)] = t.reshape(16, 16, 512).astype(ref[g].dtype)

    def wide_grad(half, ref):
        for m in range(2):
            for h in range(2):
                t = rows_by_columns(a1[:, pl.ds((m + 2 * half) * 256, 256)], b2[:, pl.ds(h * 512, 512)])
                ref[TWO][pl.ds(h * 32 + m * 16, 16)] = t.reshape(16, 16, 512).astype(ref[TWO].dtype)

    def grad_four(half, ref):
        t = rows_by_columns(a3[:, pl.ds(half * MINE, MINE)], cot[...])
        ref[FOUR][...] = t.reshape(CHUNKS, 8, WIDTH)

    own, other = refs["own"], refs["other"]
    tall_grad(a2, b3, THREE, 1, other)
    grad_four(1, other)
    first.swap()
    tall_grad(a2, b3, THREE, 0, own)
    grad_four(0, own)
    first.combine()

    backward(b3, w3c, ds2, b2)

    wide_grad(1, other)
    second.swap()
    first.relay()
    wide_grad(0, own)
    backward(b2, w2c, ds1, b1)
    second.combine()
    tall_grad(feats, b1, ONE, 1, other)
    third.swap()
    first.spread()
    tall_grad(feats, b1, ONE, 0, own)
    second.relay()
    third.combine()

    emb[core] = jnp.dot(a3[...], w4c[...], preferred_element_type=f32).astype(bf16)
    got_emb = give(emb.at[core], emb.at[core], 4, partner)

    hot_wait(rowbuf, 0, True)
    for g in range(8):
        total = rowbuf[8 * g]
        for i in range(1, 8):
            total = total + rowbuf[8 * g + i]
        rowsum[0, g] = total
    got_rows = give(rowsum.at[0], rowsum.at[1], 5, partner)
    hot_wait(carr.at[0], 1, True)
    got_carr = give(carr.at[0], carr.at[1], 6, partner)

    def select(which, block, into):
        row = lax.broadcasted_iota(i32, (ROWBLOCK, WIDTH), 0) + (block * ROWBLOCK + 1)
        for g in range(8):
            hit = row == jnp.broadcast_to(rowsum[which, g][0:1, :], (ROWBLOCK, WIDTH))
            into[:, pl.ds(g * WIDTH, WIDTH)] = jnp.where(hit, 1.0, 0.0).astype(bf16)

    blocks = OWNED // ROWBLOCK
    kept = core * (blocks // 2)

    def fetch(lo, hi, update):
        @pl.loop(lo, hi, step=2)
        def _(n):
            for k, hot_block in ((0, onehot), (1, twohot)):
                block = lax.rem(kept + n + k, blocks)
                where = tile(block, ROWBLOCK)
                select(0, block, hot_block)
                embt[...] += jnp.dot(tabt[:, where], hot_block[...], preferred_element_type=f32)
                if update:
                    delta = jnp.dot(
                        hot_block[...], carr[0].reshape(ASKED, WIDTH), preferred_element_type=f32
                    )
                    newtab[where, :] = tab[where, :] - learn_rate * delta

    def update(lo, hi):
        @pl.loop(lo, hi, step=2)
        def _(n):
            for k, hot_block in ((0, onehot), (1, twohot)):
                where = tile(kept + n + k, ROWBLOCK)
                select(1, kept + n + k, hot_block)
                delta = jnp.dot(
                    hot_block[...], carr[1].reshape(ASKED, WIDTH), preferred_element_type=f32
                )
                newtab[where, :] = newtab[where, :] - learn_rate * delta

    embt[...] = jnp.zeros_like(embt)
    fetch(0, 2, True)
    second.spread()
    third.relay()
    fetch(2, 4, True)
    first.finish()
    third.spread()
    fetch(4, 6, False)
    fetch(6, 8, False)

    for g in range(8):
        found = jnp.transpose(embt[:, pl.ds(g * WIDTH, WIDTH)]).astype(bf16)
        ebuf[pl.ds(g * 8, 8)] = found.reshape(8, SPAN, WIDTH)

    @pl.loop(1, CHUNKS, unroll=7)
    def _(j):
        s = lax.rem(me + j, CHUNKS)
        hot(ebuf.at[s], hout.at[me, core], 2, s).start()

    hout[pl.ds(me, 1), pl.ds(core, 1)] = ebuf[pl.ds(me, 1)][:, None]

    second.finish()
    got_rows.wait_recv()
    got_carr.wait_recv()
    update(0, 2)
    first.share()
    third.finish()
    update(2, 4)
    half = tile(core, OWNED // 2)
    got_table = give(newtab.at[half], newtab.at[half], 8, partner)
    first.forward()
    second.share()
    second.forward()
    first.close()
    third.share()
    hot_wait(hout.at[:, 0], 2, True)
    got_hot = give(hout.at[:, core], hout.at[:, core], 7, partner)
    third.forward()
    second.close()
    got_emb.wait_recv()
    got_table.wait_recv()
    got_hot.wait_recv()
    third.close()

    for group in (first, second, third):
        group.drain()
    for c in sent:
        c.wait_send()
    hot_wait(rowbuf, 0, False)
    hot_wait(carr.at[0], 1, False)
    hot_wait(ebuf, 2, False)


def shapes(count, types=TYPES):
    return [pltpu.VMEM((count, ROWS[g], LANES[g]), types[g]) for g in range(4)]


def outs(kind):
    sizes = [(CHUNKS, ROWS[g], LANES[g]) for g in range(4)]
    sizes[TWO] = (CHUNKS // 2, 16, 1024)
    return [kind(sizes[g], TYPES[g]) for g in range(4)]


def step(*args):
    vmem = pl.BlockSpec(memory_space=pltpu.VMEM)
    anywhere = pl.BlockSpec(memory_space=pl.ANY)
    dma = pltpu.SemaphoreType.DMA
    square = (HIDDEN, HIDDEN)
    tokens = (TOKENS, HIDDEN)
    return pl.pallas_call(
        step_kernel,
        out_shape=outs(jax.ShapeDtypeStruct) + [
            jax.ShapeDtypeStruct((CHUNKS, 2, SPAN, WIDTH), bf16),
            jax.ShapeDtypeStruct((OWNED, WIDTH), f32),
            jax.ShapeDtypeStruct((2, TOKENS, WIDTH), bf16),
        ],
        in_specs=[anywhere] * 12,
        out_specs=[vmem] * 7,
        scratch_shapes=(
            shapes(CHUNKS)
            + shapes(CHUNKS)
            + shapes(CHUNKS)
            + shapes(PLANE)
            + shapes(2 * PLANE)
            + shapes(PLANE)
            + shapes(PLANE - 1)
            + shapes(1)
            + [dma((len(STREAMS), SLOTS)), dma((len(STREAMS), SLOTS))]
            + [pltpu.VMEM((CHUNKS, 16, 512), f32), pltpu.VMEM((CHUNKS, 8, WIDTH), f32)]
            + [pltpu.VMEM(square, bf16)] * 3
            + [pltpu.VMEM((HIDDEN, WIDTH), bf16)]
            + [pltpu.VMEM(tokens, bf16)] * 4
            + [pltpu.VMEM(tokens, f32)] * 3
            + [pltpu.VMEM(tokens, bf16)] * 2
            + [
                pltpu.VMEM((TOKENS, WIDTH), bf16),
                pltpu.VMEM((OWNED, WIDTH), f32),
                pltpu.VMEM((WIDTH, OWNED), bf16),
                pltpu.VMEM((WIDTH, WIDTH), i32),
                pltpu.VMEM((CHUNKS, 8, WIDTH), i32),
                pltpu.VMEM((CHUNKS, 8, WIDTH), i32),
                pltpu.VMEM((2, 8, 8, WIDTH), i32),
                pltpu.VMEM((CHUNKS, SPAN, WIDTH), bf16),
                pltpu.VMEM((2, CHUNKS, SPAN, WIDTH), bf16),
                pltpu.VMEM((ROWBLOCK, ASKED), bf16),
                pltpu.VMEM((ROWBLOCK, ASKED), bf16),
                pltpu.VMEM((WIDTH, ASKED), f32),
                pltpu.VMEM((CHUNKS, SPAN, WIDTH), bf16),
                dma((12,)), dma((10,)), dma((10,)), dma((3,)), dma((3,)),
                pltpu.VMEM((1, 2 * SPAN, CHUNKS), i32),
                pltpu.VMEM((1, CHUNKS), i32),
                pltpu.VMEM((8, WIDTH), i32),
                pltpu.VMEM((8, WIDTH), i32),
                pltpu.VMEM((8, WIDTH), i32),
            ]
        ),
        compiler_params=pltpu.CompilerParams(
            collective_id=0, has_side_effects=True, vmem_limit_bytes=43 * 1024 * 1024
        ),
        name="step",
    )(*(pltpu.with_memory_space_constraint(a, pltpu.HBM) for a in args))


def deliver(results, factor):
    vmem = pl.BlockSpec(memory_space=pltpu.VMEM)
    pieces = 4

    def kernel(*refs):
        sources, targets, stages, sem = refs[:7], refs[7:14], refs[14:18], refs[18]
        copies = []

        def put(src, dst):
            c = pltpu.make_async_copy(src, dst, sem.at[len(copies)])
            c.start()
            copies.append(c)

        for src, dst in zip(sources[4:], targets[4:]):
            put(src, dst)
        for src, dst, stage in zip(sources, targets, stages):
            n = src.shape[0] // pieces
            for i in range(pieces):
                part = pl.ds(i * n, n)
                stage[part] = src[part].astype(f32) * factor
                put(stage.at[part], dst.at[part])
        for c in copies:
            c.wait()

    return pl.pallas_call(
        kernel,
        out_shape=[
            jax.ShapeDtypeStruct(r.shape, f32 if i < 4 else r.dtype) for i, r in enumerate(results)
        ],
        in_specs=[vmem] * 7,
        out_specs=[pl.BlockSpec(memory_space=pl.ANY)] * 7,
        scratch_shapes=[pltpu.VMEM(r.shape, f32) for r in results[:4]]
        + [pltpu.SemaphoreType.DMA((3 + 4 * pieces,))],
        compiler_params=pltpu.CompilerParams(vmem_limit_bytes=16 * 1024 * 1024),
        name="deliver",
    )(*results)


def local(
    hot_rows, hot_count, hot_cot, table, cold_ids, hash_mult, hash_add,
    layer_one, layer_two, layer_three, layer_four, cold_cot,
):
    results = step(
        hot_rows.transpose(0, 2, 1), hot_count, cold_ids.reshape(8, WIDTH),
        hash_mult.reshape(8, WIDTH), hash_add.reshape(8, WIDTH),
        layer_one, layer_two, layer_three, layer_four, cold_cot, hot_cot, table,
    )
    factor = float(cold_ids.shape[0] * lax.axis_size("dp")) ** (-0.5)
    g3, g4, g2, g1, hot_emb, new_table, cold_emb = deliver(results, factor)
    return (
        hot_emb.reshape(hot_cot.shape),
        new_table,
        cold_emb.reshape(cold_cot.shape),
        g1.reshape(layer_one.shape),
        g2.reshape(layer_two.shape),
        g3.reshape(layer_three.shape),
        g4.reshape(layer_four.shape),
    )


def solution(mesh):
    in_specs = (
        P("dp", None, None),
        P("dp", None),
        P("dp", None, None, None),
        P("dp", None),
        P("dp"),
        P(),
        P(),
        P(None, "mp"),
        P("mp", None),
        P(None, "mp"),
        P("mp", None),
        P("dp", None),
    )
    out_specs = (
        P("dp", None, None, None),
        P("dp", None),
        P("dp", None),
        P(None, "mp"),
        P("mp", None),
        P(None, "mp"),
        P("mp", None),
    )
    return jax.shard_map(local, mesh=mesh, in_specs=in_specs, out_specs=out_specs, check_vma=False)
```

```python
import jax
import jax.numpy as jnp
from jax import lax
from jax.experimental import pallas as pl
from jax.experimental.pallas import tpu as pltpu
from jax.sharding import PartitionSpec as P

MESH = pl.DeviceIdType.MESH
bf16, f32, i32 = jnp.bfloat16, jnp.float32, jnp.int32
learn_rate = 0.5
modulus = 1000003
RING = 4
PLANE = RING * RING
CHUNKS = RING * PLANE
HALF = PLANE // 2
TOKENS = 512
HIDDEN = 1024
MINE = 512
WIDTH = 128
OWNED = 4096
SPAN = 16
ASKED = CHUNKS * SPAN
ROWBLOCK = 512

THREE, FOUR, TWO, ONE = range(4)
LANES = (512, 128, 512, 512)
ROWS = (16, 8, 16, 16)
TYPES = (bf16,) * 4
DIRECT = (ONE,)
STREAMS = (
    (THREE, 0, 2, 0),
    (THREE, 2, 1, 1),
    (THREE, 3, 1, 2),
    (FOUR, 0, 1, 1),
    (TWO, 0, 2, 1),
    (TWO, 2, 1, 2),
    (TWO, 3, 1, 0),
    (ONE, 0, 2, 2),
    (ONE, 2, 1, 0),
    (ONE, 3, 1, 1),
)
SLOTS = 17


class Place:
    def __init__(self, axis):
        me = lax.axis_index("dp")
        self.core = lax.axis_index("mp")
        strides = (1, RING, RING * RING)
        self.stride = strides[axis]
        self.others = (strides[(axis + 1) % 3], strides[(axis + 2) % 3])
        self.k = lax.rem(lax.div(me, self.stride), RING)
        self.first = lax.rem(lax.div(me, self.others[0]), RING)
        self.second = lax.rem(lax.div(me, self.others[1]), RING)
        self.p = self.first * RING + self.second
        self.after = lax.rem(self.k + 1, RING)
        self.before = lax.rem(self.k + RING - 1, RING)
        self.opposite = lax.rem(self.k + 2, RING)
        self.right = me + (self.after - self.k) * self.stride
        self.left = me + (self.before - self.k) * self.stride

    def along(self, axis, j):
        at = self.second if axis else self.first
        to = lax.rem(at + j, RING)
        return lax.axis_index("dp") + (to - at) * self.others[axis], to

    def peer(self, p):
        return (
            self.k * self.stride
            + lax.div(p, RING) * self.others[0]
            + lax.rem(p, RING) * self.others[1]
        )


class Stream:
    def __init__(self, index, refs, places):
        self.grad, b0, nb, axis = STREAMS[index]
        self.place = places[axis]
        self.index = index
        self.lanes = pl.ds(b0 * WIDTH, nb * WIDTH)
        self.lane0, self.nlanes = b0 * WIDTH, nb * WIDTH
        g = self.grad
        for name in ("own", "other", "arrive", "total", "out", "near", "side", "part", "fan"):
            setattr(self, name, refs[name][g])
        self.send, self.recv = refs["send"], refs["recv"]
        self.dtype = TYPES[g]
        self.pending = []

    def view(self, ref, first, count):
        return ref.at[pl.ds(first, count), :, self.lanes]

    def outview(self, ref, first, count):
        if self.grad != TWO:
            return self.view(ref, first, count)
        half = CHUNKS // 2
        lane = pl.multiple_of(lax.div(first, half) * 512 + self.lane0, WIDTH)
        return ref.at[pl.ds(lax.rem(first, half), count), :, pl.ds(lane, self.nlanes)]

    def load(self, ref, first, count):
        return ref[pl.ds(first, count), :, self.lanes].astype(f32)

    def store(self, ref, first, count, value):
        ref[pl.ds(first, count), :, self.lanes] = value.astype(self.dtype)

    def copy(self, src, dst, slot, device):
        return pltpu.make_async_remote_copy(
            src_ref=src, dst_ref=dst,
            send_sem=self.send.at[self.index, slot], recv_sem=self.recv.at[self.index, slot],
            device_id=device, device_id_type=MESH,
        )

    def start(self, src, dst, slot, dp=None, mp=None):
        where = (
            lax.axis_index("dp") if dp is None else dp,
            self.place.core if mp is None else mp,
        )
        c = self.copy(src, dst, slot, where)
        c.start()
        self.pending.append(c)
        return c

    def swap(self):
        self.c_swap = self.start(
            self.view(self.other, 0, CHUNKS), self.view(self.arrive, 0, CHUNKS), 0,
            mp=1 - self.place.core,
        )

    def combine(self):
        self.c_swap.wait_recv()

        @pl.loop(0, CHUNKS // 8, unroll=2)
        def _(i):
            self.store(
                self.total, i * 8, 8,
                self.load(self.own, i * 8, 8) + self.load(self.arrive, i * 8, 8),
            )

        q = self.place
        base = q.opposite * PLANE
        self.c_na = self.start(
            self.view(self.total, base, HALF), self.view(self.near, 0, HALF), 1, dp=q.right
        )
        self.c_nb = self.start(
            self.view(self.total, base + HALF, HALF), self.view(self.near, HALF, HALF), 2, dp=q.left
        )
        self.c_sa = self.start(
            self.view(self.total, q.after * PLANE + HALF, HALF),
            self.view(self.side, HALF, HALF), 3, dp=q.right,
        )
        self.c_sb = self.start(
            self.view(self.total, q.before * PLANE, HALF),
            self.view(self.side, PLANE, HALF), 4, dp=q.left,
        )

    def relay(self):
        q = self.place
        low, high = q.after * PLANE, q.before * PLANE + HALF
        self.c_na.wait_recv()
        self.store(
            self.total, low, HALF, self.load(self.total, low, HALF) + self.load(self.near, 0, HALF)
        )
        self.c_ra = self.start(
            self.view(self.total, low, HALF), self.view(self.side, 0, HALF), 5, dp=q.right
        )
        self.c_nb.wait_recv()
        self.store(
            self.total, high, HALF,
            self.load(self.total, high, HALF) + self.load(self.near, HALF, HALF),
        )
        self.c_rb = self.start(
            self.view(self.total, high, HALF), self.view(self.side, PLANE + HALF, HALF), 6, dp=q.left
        )

    def spread(self):
        q = self.place
        for c in (self.c_sa, self.c_sb, self.c_ra, self.c_rb):
            c.wait_recv()

        @pl.loop(0, PLANE // 4, unroll=2)
        def _(i):
            self.store(
                self.part, i * 4, 4,
                self.load(self.total, q.k * PLANE + i * 4, 4)
                + self.load(self.side, i * 4, 4)
                + self.load(self.side, PLANE + i * 4, 4),
            )

        if self.grad in DIRECT:
            @pl.loop(1, PLANE, unroll=5)
            def _(j):
                p = lax.rem(q.p + j, PLANE)
                self.copy(
                    self.view(self.part, p, 1), self.view(self.fan, j - 1, 1), 7, (q.peer(p), q.core)
                ).start()
        else:
            for j in range(1, RING):
                dp, to = q.along(0, j)
                self.copy(
                    self.view(self.part, to * RING, RING), self.view(self.fan, (j - 1) * RING, RING),
                    7, (dp, q.core),
                ).start()

    def middle(self):
        if self.grad in DIRECT:
            return
        q = self.place
        self.wait_chunks(7, 12, True)
        mine = q.first * RING
        acc = self.load(self.part, mine, RING)
        for j in range(3):
            acc = acc + self.load(self.fan, j * RING, RING)
        self.store(self.part, mine, RING, acc)
        for j in range(1, RING):
            dp, to = q.along(1, j)
            self.copy(
                self.view(self.part, mine + to, 1), self.view(self.fan, 11 + j, 1), 15, (dp, q.core)
            ).start()

    def wait_chunks(self, slot, count, recv):
        some = self.view(self.fan, 0, count)
        sem = (self.recv if recv else self.send).at[self.index, slot]
        pltpu.make_async_copy(some, some, sem).wait()

    def finish(self):
        q = self.place
        direct = self.grad in DIRECT
        if direct:
            self.wait_chunks(7, 15, True)
        else:
            self.wait_chunks(15, 3, True)
        acc = self.load(self.part, q.p, 1)
        for i in range(0 if direct else 12, PLANE - 1):
            acc = acc + self.load(self.fan, i, 1)
        here = q.k * PLANE + q.p
        result = self.outview(self.out, here, 1)
        result[...] = acc.astype(self.dtype)
        if direct:
            @pl.loop(1, PLANE, unroll=5)
            def _(j):
                p = lax.rem(q.p + j, PLANE)
                self.copy(result, result, 8, (q.peer(p), q.core)).start()
        else:
            for j in range(1, RING):
                self.copy(result, result, 8, (q.along(1, j)[0], q.core)).start()

    def collect(self):
        if self.grad in DIRECT:
            return
        q = self.place
        self.wait_chunks(8, 3, True)
        four = self.outview(self.out, q.k * PLANE + q.first * RING, RING)
        for j in range(1, RING):
            self.copy(four, four, 16, (q.along(0, j)[0], q.core)).start()

    def share(self):
        q = self.place
        if self.grad in DIRECT:
            self.wait_chunks(8, 15, True)
        else:
            self.wait_chunks(16, 12, True)
        low = self.outview(self.out, q.k * PLANE, HALF)
        high = self.outview(self.out, q.k * PLANE + HALF, HALF)
        self.c_gl = self.start(low, low, 9, dp=q.right)
        self.c_gh = self.start(high, high, 10, dp=q.left)
        self.c_hh = self.start(high, high, 11, dp=q.right)
        self.c_hl = self.start(low, low, 12, dp=q.left)

    def forward(self):
        q = self.place
        self.c_gl.wait_recv()
        low = self.outview(self.out, q.before * PLANE, HALF)
        self.c_fl = self.start(low, low, 13, dp=q.right)
        self.c_gh.wait_recv()
        high = self.outview(self.out, q.after * PLANE + HALF, HALF)
        self.c_fh = self.start(high, high, 14, dp=q.left)

    def close(self):
        for c in (self.c_hh, self.c_hl, self.c_fl, self.c_fh):
            c.wait_recv()

    def drain(self):
        for c in self.pending:
            c.wait_send()
        if self.grad in DIRECT:
            counts = ((7, 15), (8, 15))
        else:
            counts = ((7, 12), (15, 3), (8, 3), (16, 12))
        for slot, count in counts:
            self.wait_chunks(slot, count, False)


class Group:
    def __init__(self, streams):
        self.streams = streams

    def __getattr__(self, step):
        def run():
            for s in self.streams:
                getattr(s, step)()
        return run


def rows_by_columns(a, b):
    return lax.dot_general(a, b, (((0,), (0,)), ((), ())), preferred_element_type=f32)


def times_transposed(a, b):
    return lax.dot_general(a, b, (((1,), (1,)), ((), ())), preferred_element_type=f32)


def tile(n, size=256):
    return pl.ds(pl.multiple_of(n * size, size), size)


def step_kernel(
    rows_in, count_in, ids_in, mult_in, add_in, w1, w2, w3, w4, ccot, hcot, table,
    r3, r4, r2, r1, hout, newtab, emb,
    *rest,
):
    names = ("other", "arrive", "total", "near", "side", "part", "fan")
    refs = {name: rest[4 * i : 4 * i + 4] for i, name in enumerate(names)}
    rest = rest[4 * len(names) :]
    (
        refs["send"], refs["recv"], own_large, own_four,
        w1c, w2c, w3c, w4c, feats, a1, a2, a3, ds1, ds2, ds3, b2, b3, cot,
        tab, tabt, spare, rowmsg, rowbuf, rowsum, hc, carr, onehot, twohot, embt, ebuf,
        loads, wsend, wrecv, hsend, hrecv, rows, count, ids, mult, add,
    ) = rest
    b1 = b3
    refs["out"] = (r3, r4, r2, r1)
    refs["own"] = (own_large, own_four, own_large, own_large)
    me = lax.axis_index("dp")
    core = lax.axis_index("mp")
    partner = (me, 1 - core)
    places = [Place(a) for a in range(3)]
    streams = [Stream(i, refs, places) for i in range(len(STREAMS))]
    first, second, third = Group(streams[:4]), Group(streams[4:7]), Group(streams[7:])

    load = {}
    for n, (name, src, dst) in enumerate((
        ("rows", rows_in, rows),
        ("count", count_in, count),
        ("ids", ids_in, ids),
        ("mult", mult_in, mult),
        ("add", add_in, add),
        ("w1", w1, w1c.at[:, pl.ds(0, MINE)]),
        ("w2", w2, w2c.at[pl.ds(0, MINE)]),
        ("w3", w3, w3c.at[:, pl.ds(0, MINE)]),
        ("w4", w4, w4c.at[pl.ds(0, MINE)]),
        ("hcot", hcot.at[0, :, pl.ds(pl.multiple_of(core * SPAN, SPAN), SPAN)], hc),
        ("cot", ccot.at[pl.ds(pl.multiple_of(core * TOKENS, TOKENS), TOKENS)], cot),
        ("table", table, tab),
    )):
        load[name] = pltpu.make_async_copy(src, dst, loads.at[n])
        load[name].start()

    barrier = pltpu.get_barrier_semaphore()
    pl.semaphore_signal(barrier, inc=1, device_id=partner, device_id_type=MESH)

    @pl.loop(1, CHUNKS, unroll=7)
    def _(j):
        pl.semaphore_signal(
            barrier, inc=1, device_id=(lax.rem(me + j, CHUNKS), core), device_id_type=MESH
        )

    for name in ("rows", "count", "ids", "mult", "add"):
        load[name].wait()
    slot = lax.broadcasted_iota(i32, (SPAN, CHUNKS), 0) + core * SPAN
    want = rows[0, pl.ds(pl.multiple_of(core * SPAN, SPAN), SPAN), :] + 1
    spare[...] = jnp.zeros_like(spare)
    spare[pl.ds(pl.multiple_of(lax.rem(me, 8) * SPAN, SPAN), SPAN), pl.ds(0, CHUNKS)] = jnp.where(
        slot < count[...], want, 0
    )
    want = jnp.transpose(spare[...])[:CHUNKS]
    rowmsg[...] = jnp.broadcast_to(want[:, None, :], (CHUNKS, 8, WIDTH))

    for b in range(TOKENS // WIDTH):
        line = ids[pl.ds(core * (TOKENS // WIDTH) + b, 1), :]
        column = jnp.transpose(jnp.broadcast_to(line, (WIDTH, WIDTH)))

        @pl.loop(0, HIDDEN // WIDTH, unroll=2)
        def _(j, b=b, column=column):
            h = column * mult[pl.ds(j, 1), :] + add[pl.ds(j, 1), :]
            q = (h.astype(f32) * ((1.0 - 4e-7) / modulus)).astype(i32)
            r = h - q * modulus
            r = jnp.where(r >= modulus, r - modulus, r)
            feats[pl.ds(b * WIDTH, WIDTH), tile(j, WIDTH)] = (
                r.astype(f32) * (2.0 / 1000002.0) - 1.0
            ).astype(bf16)

    pl.semaphore_wait(barrier, CHUNKS)

    sent = []

    def give(src, dst, n, device):
        c = pltpu.make_async_remote_copy(
            src_ref=src, dst_ref=dst, send_sem=wsend.at[n], recv_sem=wrecv.at[n],
            device_id=device, device_id_type=MESH,
        )
        c.start()
        sent.append(c)
        return c

    mine, theirs = pl.ds(0, MINE), pl.ds(MINE, MINE)
    load["w1"].wait()
    got1 = [
        give(w1c.at[:, pl.ds(256 * n, 256)], w1c.at[:, pl.ds(MINE + 256 * n, 256)], n, partner)
        for n in range(2)
    ]
    load["w2"].wait()
    got2 = give(w2c.at[mine], w2c.at[theirs], 9, partner)

    load["table"].wait()

    @pl.loop(0, OWNED // WIDTH, unroll=8)
    def _(n):
        tabt[:, tile(n, WIDTH)] = jnp.transpose(tab[tile(n, WIDTH), :]).astype(bf16)

    def hot_wait(ref, n, recv):
        sem = (hrecv if recv else hsend).at[n]
        part = ref.at[pl.ds(0, CHUNKS - 1)]
        pltpu.make_async_copy(part, part, sem).wait()

    def activate(pre, act, ds, columns):
        sig = 0.5 * jnp.tanh(0.5 * pre) + 0.5
        act[:, columns] = (pre * sig).astype(bf16)
        ds[:, columns] = sig + (pre * sig) * (1.0 - sig)

    def layer(src, w, act, ds, lo, hi):
        for n in range(lo, hi):
            columns = pl.ds(n * 256, 256)
            pre = jnp.dot(src[...], w[:, columns], preferred_element_type=f32)
            activate(pre, act, ds, columns)

    layer(feats, w1c, a1, ds1, 0, 2)
    load["w3"].wait()
    got3 = give(w3c.at[:, mine], w3c.at[:, theirs], 2, partner)
    load["w4"].wait()
    got4 = give(w4c.at[mine], w4c.at[theirs], 3, partner)
    got1[0].wait_recv()
    layer(feats, w1c, a1, ds1, 2, 3)
    got1[1].wait_recv()
    layer(feats, w1c, a1, ds1, 3, 4)

    load["hcot"].wait()

    def hot(src, dst, n, s):
        return pltpu.make_async_remote_copy(
            src_ref=src, dst_ref=dst, send_sem=hsend.at[n], recv_sem=hrecv.at[n],
            device_id=(s, core), device_id_type=MESH,
        )

    @pl.loop(1, CHUNKS, unroll=7)
    def _(j):
        o = lax.rem(me + j, CHUNKS)
        hot(rowmsg.at[o], rowbuf.at[me], 0, o).start()
        hot(hc.at[o], carr.at[0, me], 1, o).start()

    rowbuf[pl.ds(me, 1)] = rowmsg[pl.ds(me, 1)]
    carr[0, pl.ds(me, 1)] = hc[pl.ds(me, 1)]

    got2.wait_recv()
    layer(a1, w2c, a2, ds2, 0, 4)
    layer(a2, w3c, a3, ds3, 0, 2)
    got3.wait_recv()
    layer(a2, w3c, a3, ds3, 2, 4)
    got4.wait_recv()
    load["cot"].wait()

    def backward(src, w, ds, out):
        for n in range(4):
            columns = pl.ds(n * 256, 256)
            out[:, columns] = (times_transposed(src[...], w[columns, :]) * ds[:, columns]).astype(bf16)

    backward(cot, w4c, ds3, b3)

    def tall_grad(act, back, g, half, ref):
        for m in range(4):
            t = rows_by_columns(act[:, pl.ds(m * 256, 256)], back[:, pl.ds(half * MINE, MINE)])
            ref[g][pl.ds(m * 16, 16)] = t.reshape(16, 16, 512).astype(ref[g].dtype)

    def wide_grad(half, ref):
        for m in range(2):
            for h in range(2):
                t = rows_by_columns(a1[:, pl.ds((m + 2 * half) * 256, 256)], b2[:, pl.ds(h * 512, 512)])
                ref[TWO][pl.ds(h * 32 + m * 16, 16)] = t.reshape(16, 16, 512).astype(ref[TWO].dtype)

    def grad_four(half, ref):
        t = rows_by_columns(a3[:, pl.ds(half * MINE, MINE)], cot[...])
        ref[FOUR][...] = t.reshape(CHUNKS, 8, WIDTH).astype(ref[FOUR].dtype)

    own, other = refs["own"], refs["other"]
    tall_grad(a2, b3, THREE, 1, other)
    grad_four(1, other)
    first.swap()
    tall_grad(a2, b3, THREE, 0, own)
    grad_four(0, own)
    backward(b3, w3c, ds2, b2)
    first.combine()
    wide_grad(1, other)
    second.swap()
    wide_grad(0, own)
    backward(b2, w2c, ds1, b1)
    first.relay()
    second.combine()
    tall_grad(feats, b1, ONE, 1, other)
    third.swap()
    tall_grad(feats, b1, ONE, 0, own)

    emb[core] = jnp.dot(a3[...], w4c[...], preferred_element_type=f32).astype(bf16)
    got_emb = give(emb.at[core], emb.at[core], 4, partner)
    first.spread()
    second.relay()
    third.combine()

    hot_wait(rowbuf, 0, True)
    for g in range(8):
        total = rowbuf[8 * g]
        for i in range(1, 8):
            total = total + rowbuf[8 * g + i]
        rowsum[0, g] = total
    got_rows = give(rowsum.at[0], rowsum.at[1], 5, partner)
    hot_wait(carr.at[0], 1, True)
    got_carr = give(carr.at[0], carr.at[1], 6, partner)

    def select(which, block, into):
        row = lax.broadcasted_iota(i32, (ROWBLOCK, WIDTH), 0) + (block * ROWBLOCK + 1)
        for g in range(8):
            hit = row == jnp.broadcast_to(rowsum[which, g][0:1, :], (ROWBLOCK, WIDTH))
            into[:, pl.ds(g * WIDTH, WIDTH)] = jnp.where(hit, 1.0, 0.0).astype(bf16)

    blocks = OWNED // ROWBLOCK
    kept = core * (blocks // 2)

    def fetch(lo, hi, update):
        @pl.loop(lo, hi, step=2)
        def _(n):
            for k, hot_block in ((0, onehot), (1, twohot)):
                block = lax.rem(kept + n + k, blocks)
                where = tile(block, ROWBLOCK)
                select(0, block, hot_block)
                embt[...] += jnp.dot(tabt[:, where], hot_block[...], preferred_element_type=f32)
                if update:
                    delta = jnp.dot(
                        hot_block[...], carr[0].reshape(ASKED, WIDTH), preferred_element_type=f32
                    )
                    newtab[where, :] = tab[where, :] - learn_rate * delta

    def update(lo, hi):
        @pl.loop(lo, hi, step=2)
        def _(n):
            for k, hot_block in ((0, onehot), (1, twohot)):
                where = tile(kept + n + k, ROWBLOCK)
                select(1, kept + n + k, hot_block)
                delta = jnp.dot(
                    hot_block[...], carr[1].reshape(ASKED, WIDTH), preferred_element_type=f32
                )
                newtab[where, :] = newtab[where, :] - learn_rate * delta

    embt[...] = jnp.zeros_like(embt)
    fetch(0, 2, True)
    first.middle()
    second.spread()
    third.relay()
    fetch(2, 4, True)
    fetch(4, 6, False)
    first.finish()
    second.middle()
    third.spread()
    fetch(6, 8, False)

    for g in range(8):
        found = jnp.transpose(embt[:, pl.ds(g * WIDTH, WIDTH)]).astype(bf16)
        ebuf[pl.ds(g * 8, 8)] = found.reshape(8, SPAN, WIDTH)

    @pl.loop(1, CHUNKS, unroll=7)
    def _(j):
        s = lax.rem(me + j, CHUNKS)
        hot(ebuf.at[s], hout.at[me, core], 2, s).start()

    hout[pl.ds(me, 1), pl.ds(core, 1)] = ebuf[pl.ds(me, 1)][:, None]

    second.finish()
    first.collect()
    got_rows.wait_recv()
    got_carr.wait_recv()
    update(0, 2)
    third.finish()
    second.collect()
    first.share()
    update(2, 4)
    half = tile(core, OWNED // 2)
    got_table = give(newtab.at[half], newtab.at[half], 8, partner)
    second.share()
    first.forward()
    third.share()
    hot_wait(hout.at[:, 0], 2, True)
    got_hot = give(hout.at[:, core], hout.at[:, core], 7, partner)
    second.forward()
    third.forward()
    first.close()
    second.close()
    got_emb.wait_recv()
    got_table.wait_recv()
    got_hot.wait_recv()
    third.close()

    for group in (first, second, third):
        group.drain()
    for c in sent:
        c.wait_send()
    hot_wait(rowbuf, 0, False)
    hot_wait(carr.at[0], 1, False)
    hot_wait(ebuf, 2, False)


def shapes(count, types=TYPES):
    return [pltpu.VMEM((count, ROWS[g], LANES[g]), types[g]) for g in range(4)]


def outs(kind):
    sizes = [(CHUNKS, ROWS[g], LANES[g]) for g in range(4)]
    sizes[TWO] = (CHUNKS // 2, 16, 1024)
    return [kind(sizes[g], TYPES[g]) for g in range(4)]


def step(*args):
    vmem = pl.BlockSpec(memory_space=pltpu.VMEM)
    anywhere = pl.BlockSpec(memory_space=pl.ANY)
    dma = pltpu.SemaphoreType.DMA
    square = (HIDDEN, HIDDEN)
    tokens = (TOKENS, HIDDEN)
    return pl.pallas_call(
        step_kernel,
        out_shape=outs(jax.ShapeDtypeStruct) + [
            jax.ShapeDtypeStruct((CHUNKS, 2, SPAN, WIDTH), bf16),
            jax.ShapeDtypeStruct((OWNED, WIDTH), f32),
            jax.ShapeDtypeStruct((2, TOKENS, WIDTH), bf16),
        ],
        in_specs=[anywhere] * 12,
        out_specs=[vmem] * 7,
        scratch_shapes=(
            shapes(CHUNKS)
            + shapes(CHUNKS)
            + shapes(CHUNKS)
            + shapes(PLANE)
            + shapes(2 * PLANE)
            + shapes(PLANE)
            + shapes(PLANE - 1)
            + [dma((len(STREAMS), SLOTS)), dma((len(STREAMS), SLOTS))]
            + [pltpu.VMEM((CHUNKS, 16, 512), f32), pltpu.VMEM((CHUNKS, 8, WIDTH), f32)]
            + [pltpu.VMEM(square, bf16)] * 3
            + [pltpu.VMEM((HIDDEN, WIDTH), bf16)]
            + [pltpu.VMEM(tokens, bf16)] * 4
            + [pltpu.VMEM(tokens, f32)] * 3
            + [pltpu.VMEM(tokens, bf16)] * 2
            + [
                pltpu.VMEM((TOKENS, WIDTH), bf16),
                pltpu.VMEM((OWNED, WIDTH), f32),
                pltpu.VMEM((WIDTH, OWNED), bf16),
                pltpu.VMEM((WIDTH, WIDTH), i32),
                pltpu.VMEM((CHUNKS, 8, WIDTH), i32),
                pltpu.VMEM((CHUNKS, 8, WIDTH), i32),
                pltpu.VMEM((2, 8, 8, WIDTH), i32),
                pltpu.VMEM((CHUNKS, SPAN, WIDTH), bf16),
                pltpu.VMEM((2, CHUNKS, SPAN, WIDTH), bf16),
                pltpu.VMEM((ROWBLOCK, ASKED), bf16),
                pltpu.VMEM((ROWBLOCK, ASKED), bf16),
                pltpu.VMEM((WIDTH, ASKED), f32),
                pltpu.VMEM((CHUNKS, SPAN, WIDTH), bf16),
                dma((12,)), dma((10,)), dma((10,)), dma((3,)), dma((3,)),
                pltpu.VMEM((1, 2 * SPAN, CHUNKS), i32),
                pltpu.VMEM((1, CHUNKS), i32),
                pltpu.VMEM((8, WIDTH), i32),
                pltpu.VMEM((8, WIDTH), i32),
                pltpu.VMEM((8, WIDTH), i32),
            ]
        ),
        compiler_params=pltpu.CompilerParams(
            collective_id=0, has_side_effects=True, vmem_limit_bytes=43 * 1024 * 1024
        ),
        name="step",
    )(*(pltpu.with_memory_space_constraint(a, pltpu.HBM) for a in args))


def deliver(results, factor):
    vmem = pl.BlockSpec(memory_space=pltpu.VMEM)
    pieces = 4

    def kernel(*refs):
        sources, targets, stages, sem = refs[:7], refs[7:14], refs[14:18], refs[18]
        copies = []

        def put(src, dst):
            c = pltpu.make_async_copy(src, dst, sem.at[len(copies)])
            c.start()
            copies.append(c)

        for src, dst in zip(sources[4:], targets[4:]):
            put(src, dst)
        for src, dst, stage in zip(sources, targets, stages):
            n = src.shape[0] // pieces
            for i in range(pieces):
                part = pl.ds(i * n, n)
                stage[part] = src[part].astype(f32) * factor
                put(stage.at[part], dst.at[part])
        for c in copies:
            c.wait()

    return pl.pallas_call(
        kernel,
        out_shape=[
            jax.ShapeDtypeStruct(r.shape, f32 if i < 4 else r.dtype) for i, r in enumerate(results)
        ],
        in_specs=[vmem] * 7,
        out_specs=[pl.BlockSpec(memory_space=pl.ANY)] * 7,
        scratch_shapes=[pltpu.VMEM(r.shape, f32) for r in results[:4]]
        + [pltpu.SemaphoreType.DMA((3 + 4 * pieces,))],
        compiler_params=pltpu.CompilerParams(vmem_limit_bytes=16 * 1024 * 1024),
        name="deliver",
    )(*results)


def local(
    hot_rows, hot_count, hot_cot, table, cold_ids, hash_mult, hash_add,
    layer_one, layer_two, layer_three, layer_four, cold_cot,
):
    results = step(
        hot_rows.transpose(0, 2, 1), hot_count, cold_ids.reshape(8, WIDTH),
        hash_mult.reshape(8, WIDTH), hash_add.reshape(8, WIDTH),
        layer_one, layer_two, layer_three, layer_four, cold_cot, hot_cot, table,
    )
    factor = float(cold_ids.shape[0] * lax.axis_size("dp")) ** (-0.5)
    g3, g4, g2, g1, hot_emb, new_table, cold_emb = deliver(results, factor)
    return (
        hot_emb.reshape(hot_cot.shape),
        new_table,
        cold_emb.reshape(cold_cot.shape),
        g1.reshape(layer_one.shape),
        g2.reshape(layer_two.shape),
        g3.reshape(layer_three.shape),
        g4.reshape(layer_four.shape),
    )


def solution(mesh):
    in_specs = (
        P("dp", None, None),
        P("dp", None),
        P("dp", None, None, None),
        P("dp", None),
        P("dp"),
        P(),
        P(),
        P(None, "mp"),
        P("mp", None),
        P(None, "mp"),
        P("mp", None),
        P("dp", None),
    )
    out_specs = (
        P("dp", None, None, None),
        P("dp", None),
        P("dp", None),
        P(None, "mp"),
        P("mp", None),
        P(None, "mp"),
        P("mp", None),
    )
    return jax.shard_map(local, mesh=mesh, in_specs=in_specs, out_specs=out_specs, check_vma=False)
```

```python
import jax
import jax.numpy as jnp
from jax import lax
from jax.experimental import pallas as pl
from jax.experimental.pallas import tpu as pltpu
from jax.sharding import PartitionSpec as P

MESH = pl.DeviceIdType.MESH
bf16, f32, i32 = jnp.bfloat16, jnp.float32, jnp.int32
learn_rate = 0.5
modulus = 1000003
RING = 4
PLANE = RING * RING
CHUNKS = RING * PLANE
HALF = PLANE // 2
TOKENS = 512
HIDDEN = 1024
MINE = 512
WIDTH = 128
OWNED = 4096
SPAN = 16
ASKED = CHUNKS * SPAN
ROWBLOCK = 512

THREE, FOUR, TWO, ONE = range(4)
LANES = (512, 128, 512, 512)
ROWS = (16, 8, 16, 16)
TYPES = (bf16,) * 4
DIRECT = (ONE,)
STREAMS = (
    (THREE, 0, 2, 0),
    (THREE, 2, 1, 1),
    (THREE, 3, 1, 2),
    (FOUR, 0, 1, 1),
    (TWO, 0, 2, 1),
    (TWO, 2, 1, 2),
    (TWO, 3, 1, 0),
    (ONE, 0, 2, 2),
    (ONE, 2, 1, 0),
    (ONE, 3, 1, 1),
)
SLOTS = 17


class Place:
    def __init__(self, axis):
        me = lax.axis_index("dp")
        self.core = lax.axis_index("mp")
        strides = (1, RING, RING * RING)
        self.stride = strides[axis]
        self.others = (strides[(axis + 1) % 3], strides[(axis + 2) % 3])
        self.k = lax.rem(lax.div(me, self.stride), RING)
        self.first = lax.rem(lax.div(me, self.others[0]), RING)
        self.second = lax.rem(lax.div(me, self.others[1]), RING)
        self.p = self.first * RING + self.second
        self.after = lax.rem(self.k + 1, RING)
        self.before = lax.rem(self.k + RING - 1, RING)
        self.opposite = lax.rem(self.k + 2, RING)
        self.right = me + (self.after - self.k) * self.stride
        self.left = me + (self.before - self.k) * self.stride

    def along(self, axis, j):
        at = self.second if axis else self.first
        to = lax.rem(at + j, RING)
        return lax.axis_index("dp") + (to - at) * self.others[axis], to

    def peer(self, p):
        return (
            self.k * self.stride
            + lax.div(p, RING) * self.others[0]
            + lax.rem(p, RING) * self.others[1]
        )


class Stream:
    def __init__(self, index, refs, places):
        self.grad, b0, nb, axis = STREAMS[index]
        self.place = places[axis]
        self.index = index
        self.lanes = pl.ds(b0 * WIDTH, nb * WIDTH)
        self.lane0, self.nlanes = b0 * WIDTH, nb * WIDTH
        g = self.grad
        for name in ("own", "other", "arrive", "total", "out", "near", "side", "part", "fan"):
            setattr(self, name, refs[name][g])
        self.send, self.recv = refs["send"], refs["recv"]
        self.dtype = TYPES[g]
        self.pending = []

    def view(self, ref, first, count):
        return ref.at[pl.ds(first, count), :, self.lanes]

    def outview(self, ref, first, count):
        if self.grad != TWO:
            return self.view(ref, first, count)
        half = CHUNKS // 2
        lane = pl.multiple_of(lax.div(first, half) * 512 + self.lane0, WIDTH)
        return ref.at[pl.ds(lax.rem(first, half), count), :, pl.ds(lane, self.nlanes)]

    def load(self, ref, first, count):
        return ref[pl.ds(first, count), :, self.lanes].astype(f32)

    def store(self, ref, first, count, value):
        ref[pl.ds(first, count), :, self.lanes] = value.astype(self.dtype)

    def copy(self, src, dst, slot, device):
        return pltpu.make_async_remote_copy(
            src_ref=src, dst_ref=dst,
            send_sem=self.send.at[self.index, slot], recv_sem=self.recv.at[self.index, slot],
            device_id=device, device_id_type=MESH,
        )

    def start(self, src, dst, slot, dp=None, mp=None):
        where = (
            lax.axis_index("dp") if dp is None else dp,
            self.place.core if mp is None else mp,
        )
        c = self.copy(src, dst, slot, where)
        c.start()
        self.pending.append(c)
        return c

    def swap(self):
        self.c_swap = self.start(
            self.view(self.other, 0, CHUNKS), self.view(self.arrive, 0, CHUNKS), 0,
            mp=1 - self.place.core,
        )

    def combine(self):
        self.c_swap.wait_recv()

        @pl.loop(0, CHUNKS // 8, unroll=2)
        def _(i):
            self.store(
                self.total, i * 8, 8,
                self.load(self.own, i * 8, 8) + self.load(self.arrive, i * 8, 8),
            )

        q = self.place
        base = q.opposite * PLANE
        self.c_na = self.start(
            self.view(self.total, base, HALF), self.view(self.near, 0, HALF), 1, dp=q.right
        )
        self.c_nb = self.start(
            self.view(self.total, base + HALF, HALF), self.view(self.near, HALF, HALF), 2, dp=q.left
        )
        self.c_sa = self.start(
            self.view(self.total, q.after * PLANE + HALF, HALF),
            self.view(self.side, HALF, HALF), 3, dp=q.right,
        )
        self.c_sb = self.start(
            self.view(self.total, q.before * PLANE, HALF),
            self.view(self.side, PLANE, HALF), 4, dp=q.left,
        )

    def relay(self):
        q = self.place
        low, high = q.after * PLANE, q.before * PLANE + HALF
        self.c_na.wait_recv()
        self.store(
            self.total, low, HALF, self.load(self.total, low, HALF) + self.load(self.near, 0, HALF)
        )
        self.c_ra = self.start(
            self.view(self.total, low, HALF), self.view(self.side, 0, HALF), 5, dp=q.right
        )
        self.c_nb.wait_recv()
        self.store(
            self.total, high, HALF,
            self.load(self.total, high, HALF) + self.load(self.near, HALF, HALF),
        )
        self.c_rb = self.start(
            self.view(self.total, high, HALF), self.view(self.side, PLANE + HALF, HALF), 6, dp=q.left
        )

    def spread(self):
        q = self.place
        for c in (self.c_sa, self.c_sb, self.c_ra, self.c_rb):
            c.wait_recv()

        @pl.loop(0, PLANE // 4, unroll=2)
        def _(i):
            self.store(
                self.part, i * 4, 4,
                self.load(self.total, q.k * PLANE + i * 4, 4)
                + self.load(self.side, i * 4, 4)
                + self.load(self.side, PLANE + i * 4, 4),
            )

        if self.grad in DIRECT:
            @pl.loop(1, PLANE, unroll=5)
            def _(j):
                p = lax.rem(q.p + j, PLANE)
                self.copy(
                    self.view(self.part, p, 1), self.view(self.fan, j - 1, 1), 7, (q.peer(p), q.core)
                ).start()
        else:
            for j in range(1, RING):
                dp, to = q.along(0, j)
                self.copy(
                    self.view(self.part, to * RING, RING), self.view(self.fan, (j - 1) * RING, RING),
                    7, (dp, q.core),
                ).start()

    def middle(self):
        if self.grad in DIRECT:
            return
        q = self.place
        self.wait_chunks(7, 12, True)
        mine = q.first * RING
        acc = self.load(self.part, mine, RING)
        for j in range(3):
            acc = acc + self.load(self.fan, j * RING, RING)
        self.store(self.part, mine, RING, acc)
        for j in range(1, RING):
            dp, to = q.along(1, j)
            self.copy(
                self.view(self.part, mine + to, 1), self.view(self.fan, 11 + j, 1), 15, (dp, q.core)
            ).start()

    def wait_chunks(self, slot, count, recv):
        some = self.view(self.fan, 0, count)
        sem = (self.recv if recv else self.send).at[self.index, slot]
        pltpu.make_async_copy(some, some, sem).wait()

    def finish(self):
        q = self.place
        direct = self.grad in DIRECT
        if direct:
            self.wait_chunks(7, 15, True)
        else:
            self.wait_chunks(15, 3, True)
        acc = self.load(self.part, q.p, 1)
        for i in range(0 if direct else 12, PLANE - 1):
            acc = acc + self.load(self.fan, i, 1)
        here = q.k * PLANE + q.p
        result = self.outview(self.out, here, 1)
        result[...] = acc.astype(self.dtype)
        if direct:
            @pl.loop(1, PLANE, unroll=5)
            def _(j):
                p = lax.rem(q.p + j, PLANE)
                self.copy(result, result, 8, (q.peer(p), q.core)).start()
        else:
            for j in range(1, RING):
                self.copy(result, result, 8, (q.along(1, j)[0], q.core)).start()

    def collect(self):
        if self.grad in DIRECT:
            return
        q = self.place
        self.wait_chunks(8, 3, True)
        four = self.outview(self.out, q.k * PLANE + q.first * RING, RING)
        for j in range(1, RING):
            self.copy(four, four, 16, (q.along(0, j)[0], q.core)).start()

    def share(self):
        q = self.place
        if self.grad in DIRECT:
            self.wait_chunks(8, 15, True)
        else:
            self.wait_chunks(16, 12, True)
        low = self.outview(self.out, q.k * PLANE, HALF)
        high = self.outview(self.out, q.k * PLANE + HALF, HALF)
        self.c_gl = self.start(low, low, 9, dp=q.right)
        self.c_gh = self.start(high, high, 10, dp=q.left)
        self.c_hh = self.start(high, high, 11, dp=q.right)
        self.c_hl = self.start(low, low, 12, dp=q.left)

    def forward(self):
        q = self.place
        self.c_gl.wait_recv()
        low = self.outview(self.out, q.before * PLANE, HALF)
        self.c_fl = self.start(low, low, 13, dp=q.right)
        self.c_gh.wait_recv()
        high = self.outview(self.out, q.after * PLANE + HALF, HALF)
        self.c_fh = self.start(high, high, 14, dp=q.left)

    def close(self):
        for c in (self.c_hh, self.c_hl, self.c_fl, self.c_fh):
            c.wait_recv()

    def drain(self):
        for c in self.pending:
            c.wait_send()
        if self.grad in DIRECT:
            counts = ((7, 15), (8, 15))
        else:
            counts = ((7, 12), (15, 3), (8, 3), (16, 12))
        for slot, count in counts:
            self.wait_chunks(slot, count, False)


class Group:
    def __init__(self, streams):
        self.streams = streams

    def __getattr__(self, step):
        def run():
            for s in self.streams:
                getattr(s, step)()
        return run


def rows_by_columns(a, b):
    return lax.dot_general(a, b, (((0,), (0,)), ((), ())), preferred_element_type=f32)


def times_transposed(a, b):
    return lax.dot_general(a, b, (((1,), (1,)), ((), ())), preferred_element_type=f32)


def tile(n, size=256):
    return pl.ds(pl.multiple_of(n * size, size), size)


def step_kernel(
    rows_in, count_in, ids_in, mult_in, add_in, w1, w2, w3, w4, ccot, hcot, table,
    r3, r4, r2, r1, hout, newtab, emb,
    *rest,
):
    names = ("other", "arrive", "total", "near", "side", "part", "fan")
    refs = {name: rest[4 * i : 4 * i + 4] for i, name in enumerate(names)}
    rest = rest[4 * len(names) :]
    (
        refs["send"], refs["recv"], own_large, own_four,
        w1c, w2c, w3c, w4c, feats, a1, a2, a3, ds1, ds2, ds3, b2, b3, cot,
        tab, tabt, spare, rowmsg, rowbuf, rowsum, hc, carr, onehot, twohot, embt, ebuf,
        loads, wsend, wrecv, hsend, hrecv, rows, count, ids, mult, add,
    ) = rest
    b1 = b3
    refs["out"] = (r3, r4, r2, r1)
    refs["own"] = (own_large, own_four, own_large, own_large)
    me = lax.axis_index("dp")
    core = lax.axis_index("mp")
    partner = (me, 1 - core)
    places = [Place(a) for a in range(3)]
    streams = [Stream(i, refs, places) for i in range(len(STREAMS))]
    first, second, third = Group(streams[:4]), Group(streams[4:7]), Group(streams[7:])

    load = {}
    for n, (name, src, dst) in enumerate((
        ("rows", rows_in, rows),
        ("count", count_in, count),
        ("ids", ids_in, ids),
        ("mult", mult_in, mult),
        ("add", add_in, add),
        ("w1", w1, w1c.at[:, pl.ds(0, MINE)]),
        ("w2", w2, w2c.at[pl.ds(0, MINE)]),
        ("w3", w3, w3c.at[:, pl.ds(0, MINE)]),
        ("w4", w4, w4c.at[pl.ds(0, MINE)]),
        ("hcot", hcot.at[0, :, pl.ds(pl.multiple_of(core * SPAN, SPAN), SPAN)], hc),
        ("cot", ccot.at[pl.ds(pl.multiple_of(core * TOKENS, TOKENS), TOKENS)], cot),
        ("table", table, tab),
    )):
        load[name] = pltpu.make_async_copy(src, dst, loads.at[n])
        load[name].start()

    barrier = pltpu.get_barrier_semaphore()
    pl.semaphore_signal(barrier, inc=1, device_id=partner, device_id_type=MESH)

    @pl.loop(1, CHUNKS, unroll=7)
    def _(j):
        pl.semaphore_signal(
            barrier, inc=1, device_id=(lax.rem(me + j, CHUNKS), core), device_id_type=MESH
        )

    for name in ("rows", "count", "ids", "mult", "add"):
        load[name].wait()
    slot = lax.broadcasted_iota(i32, (SPAN, CHUNKS), 0) + core * SPAN
    want = rows[0, pl.ds(pl.multiple_of(core * SPAN, SPAN), SPAN), :] + 1
    spare[...] = jnp.zeros_like(spare)
    spare[pl.ds(pl.multiple_of(lax.rem(me, 8) * SPAN, SPAN), SPAN), pl.ds(0, CHUNKS)] = jnp.where(
        slot < count[...], want, 0
    )
    want = jnp.transpose(spare[...])[:CHUNKS]
    rowmsg[...] = jnp.broadcast_to(want[:, None, :], (CHUNKS, 8, WIDTH))

    def hash_block(b):
        line = ids[pl.ds(core * (TOKENS // WIDTH) + b, 1), :]
        column = jnp.transpose(jnp.broadcast_to(line, (WIDTH, WIDTH)))

        @pl.loop(0, HIDDEN // WIDTH, unroll=2)
        def _(j):
            h = column * mult[pl.ds(j, 1), :] + add[pl.ds(j, 1), :]
            q = (h.astype(f32) * ((1.0 - 4e-7) / modulus)).astype(i32)
            r = h - q * modulus
            r = jnp.where(r >= modulus, r - modulus, r)
            feats[pl.ds(b * WIDTH, WIDTH), tile(j, WIDTH)] = (
                r.astype(f32) * (2.0 / 1000002.0) - 1.0
            ).astype(bf16)

    hash_block(0)
    hash_block(1)
    pl.semaphore_wait(barrier, CHUNKS)

    sent = []

    def give(src, dst, n, device):
        c = pltpu.make_async_remote_copy(
            src_ref=src, dst_ref=dst, send_sem=wsend.at[n], recv_sem=wrecv.at[n],
            device_id=device, device_id_type=MESH,
        )
        c.start()
        sent.append(c)
        return c

    mine, theirs = pl.ds(0, MINE), pl.ds(MINE, MINE)
    load["w1"].wait()
    got1 = [
        give(w1c.at[:, pl.ds(256 * n, 256)], w1c.at[:, pl.ds(MINE + 256 * n, 256)], n, partner)
        for n in range(2)
    ]
    load["w2"].wait()
    got2 = give(w2c.at[mine], w2c.at[theirs], 9, partner)
    hash_block(2)
    hash_block(3)

    def hot_wait(ref, n, recv):
        sem = (hrecv if recv else hsend).at[n]
        part = ref.at[pl.ds(0, CHUNKS - 1)]
        pltpu.make_async_copy(part, part, sem).wait()

    def activate(pre, act, ds, rows, columns):
        sig = 0.5 * jnp.tanh(0.5 * pre) + 0.5
        act[rows, columns] = (pre * sig).astype(bf16)
        ds[rows, columns] = sig + (pre * sig) * (1.0 - sig)

    def layer(src, w, act, ds, lo, hi):
        last = None
        for n in range(lo, hi):
            for h in range(2):
                at = (pl.ds(h * 256, 256), pl.ds(n * 256, 256))
                pre = jnp.dot(src[at[0], :], w[:, at[1]], preferred_element_type=f32)
                if last is not None:
                    activate(last[0], act, ds, *last[1])
                last = (pre, at)
        activate(last[0], act, ds, *last[1])

    layer(feats, w1c, a1, ds1, 0, 2)
    load["w3"].wait()
    got3 = give(w3c.at[:, mine], w3c.at[:, theirs], 2, partner)
    load["w4"].wait()
    got4 = give(w4c.at[mine], w4c.at[theirs], 3, partner)
    load["table"].wait()

    @pl.loop(0, OWNED // WIDTH, unroll=8)
    def _(n):
        tabt[:, tile(n, WIDTH)] = jnp.transpose(tab[tile(n, WIDTH), :]).astype(bf16)

    got1[0].wait_recv()
    layer(feats, w1c, a1, ds1, 2, 3)
    got1[1].wait_recv()
    layer(feats, w1c, a1, ds1, 3, 4)

    load["hcot"].wait()

    def hot(src, dst, n, s):
        return pltpu.make_async_remote_copy(
            src_ref=src, dst_ref=dst, send_sem=hsend.at[n], recv_sem=hrecv.at[n],
            device_id=(s, core), device_id_type=MESH,
        )

    @pl.loop(1, CHUNKS, unroll=7)
    def _(j):
        o = lax.rem(me + j, CHUNKS)
        hot(rowmsg.at[o], rowbuf.at[me], 0, o).start()
        hot(hc.at[o], carr.at[0, me], 1, o).start()

    rowbuf[pl.ds(me, 1)] = rowmsg[pl.ds(me, 1)]
    carr[0, pl.ds(me, 1)] = hc[pl.ds(me, 1)]

    got2.wait_recv()
    layer(a1, w2c, a2, ds2, 0, 4)
    layer(a2, w3c, a3, ds3, 0, 2)
    got3.wait_recv()
    layer(a2, w3c, a3, ds3, 2, 4)
    got4.wait_recv()
    load["cot"].wait()

    def backward(src, w, ds, out):
        for n in range(4):
            columns = pl.ds(n * 256, 256)
            out[:, columns] = (times_transposed(src[...], w[columns, :]) * ds[:, columns]).astype(bf16)

    backward(cot, w4c, ds3, b3)

    def tall_grad(act, back, g, half, ref):
        for m in range(4):
            t = rows_by_columns(act[:, pl.ds(m * 256, 256)], back[:, pl.ds(half * MINE, MINE)])
            ref[g][pl.ds(m * 16, 16)] = t.reshape(16, 16, 512).astype(ref[g].dtype)

    def wide_grad(half, ref):
        for m in range(2):
            for h in range(2):
                t = rows_by_columns(a1[:, pl.ds((m + 2 * half) * 256, 256)], b2[:, pl.ds(h * 512, 512)])
                ref[TWO][pl.ds(h * 32 + m * 16, 16)] = t.reshape(16, 16, 512).astype(ref[TWO].dtype)

    def grad_four():
        t = rows_by_columns(cot[...], a3[...])
        for half, ref in ((1, other), (0, own)):
            part = jnp.transpose(t[:, half * MINE : (half + 1) * MINE])
            ref[FOUR][...] = part.reshape(CHUNKS, 8, WIDTH).astype(ref[FOUR].dtype)

    own, other = refs["own"], refs["other"]
    tall_grad(a2, b3, THREE, 1, other)
    Group(streams[:3]).swap()
    grad_four()
    streams[3].swap()
    tall_grad(a2, b3, THREE, 0, own)
    backward(b3, w3c, ds2, b2)
    first.combine()
    wide_grad(1, other)
    second.swap()
    wide_grad(0, own)
    backward(b2, w2c, ds1, b1)
    first.relay()
    second.combine()
    tall_grad(feats, b1, ONE, 1, other)
    third.swap()
    tall_grad(feats, b1, ONE, 0, own)

    emb[core] = jnp.dot(a3[...], w4c[...], preferred_element_type=f32).astype(bf16)
    got_emb = give(emb.at[core], emb.at[core], 4, partner)
    first.spread()
    second.relay()
    third.combine()

    hot_wait(rowbuf, 0, True)
    for g in range(8):
        total = rowbuf[8 * g]
        for i in range(1, 8):
            total = total + rowbuf[8 * g + i]
        rowsum[0, g] = total
    got_rows = give(rowsum.at[0], rowsum.at[1], 5, partner)
    hot_wait(carr.at[0], 1, True)
    got_carr = give(carr.at[0], carr.at[1], 6, partner)

    def select(which, block, into):
        row = lax.broadcasted_iota(i32, (ROWBLOCK, WIDTH), 0) + (block * ROWBLOCK + 1)
        for g in range(8):
            hit = row == jnp.broadcast_to(rowsum[which, g][0:1, :], (ROWBLOCK, WIDTH))
            into[:, pl.ds(g * WIDTH, WIDTH)] = jnp.where(hit, 1.0, 0.0).astype(bf16)

    blocks = OWNED // ROWBLOCK
    kept = core * (blocks // 2)

    def fetch(lo, hi, update):
        @pl.loop(lo, hi, step=2)
        def _(n):
            for k, hot_block in ((0, onehot), (1, twohot)):
                block = lax.rem(kept + n + k, blocks)
                where = tile(block, ROWBLOCK)
                select(0, block, hot_block)
                embt[...] += jnp.dot(tabt[:, where], hot_block[...], preferred_element_type=f32)
                if update:
                    delta = jnp.dot(
                        hot_block[...], carr[0].reshape(ASKED, WIDTH), preferred_element_type=f32
                    )
                    newtab[where, :] = tab[where, :] - learn_rate * delta

    def update(lo, hi):
        @pl.loop(lo, hi, step=2)
        def _(n):
            for k, hot_block in ((0, onehot), (1, twohot)):
                where = tile(kept + n + k, ROWBLOCK)
                select(1, kept + n + k, hot_block)
                delta = jnp.dot(
                    hot_block[...], carr[1].reshape(ASKED, WIDTH), preferred_element_type=f32
                )
                newtab[where, :] = newtab[where, :] - learn_rate * delta

    embt[...] = jnp.zeros_like(embt)
    fetch(0, 2, True)
    first.middle()
    second.spread()
    third.relay()
    fetch(2, 4, True)
    fetch(4, 6, False)
    first.finish()
    second.middle()
    third.spread()
    fetch(6, 8, False)

    for g in range(8):
        found = jnp.transpose(embt[:, pl.ds(g * WIDTH, WIDTH)]).astype(bf16)
        ebuf[pl.ds(g * 8, 8)] = found.reshape(8, SPAN, WIDTH)

    @pl.loop(1, CHUNKS, unroll=7)
    def _(j):
        s = lax.rem(me + j, CHUNKS)
        hot(ebuf.at[s], hout.at[me, core], 2, s).start()

    hout[pl.ds(me, 1), pl.ds(core, 1)] = ebuf[pl.ds(me, 1)][:, None]

    second.finish()
    first.collect()
    got_rows.wait_recv()
    got_carr.wait_recv()
    update(0, 2)
    third.finish()
    second.collect()
    first.share()
    update(2, 4)
    half = tile(core, OWNED // 2)
    got_table = give(newtab.at[half], newtab.at[half], 8, partner)
    second.share()
    first.forward()
    third.share()
    hot_wait(hout.at[:, 0], 2, True)
    got_hot = give(hout.at[:, core], hout.at[:, core], 7, partner)
    second.forward()
    third.forward()
    first.close()
    second.close()
    got_emb.wait_recv()
    got_table.wait_recv()
    got_hot.wait_recv()
    third.close()

    for group in (first, second, third):
        group.drain()
    for c in sent:
        c.wait_send()
    hot_wait(rowbuf, 0, False)
    hot_wait(carr.at[0], 1, False)
    hot_wait(ebuf, 2, False)


def shapes(count, types=TYPES):
    return [pltpu.VMEM((count, ROWS[g], LANES[g]), types[g]) for g in range(4)]


def outs(kind):
    sizes = [(CHUNKS, ROWS[g], LANES[g]) for g in range(4)]
    sizes[TWO] = (CHUNKS // 2, 16, 1024)
    return [kind(sizes[g], TYPES[g]) for g in range(4)]


def step(*args):
    vmem = pl.BlockSpec(memory_space=pltpu.VMEM)
    anywhere = pl.BlockSpec(memory_space=pl.ANY)
    dma = pltpu.SemaphoreType.DMA
    square = (HIDDEN, HIDDEN)
    tokens = (TOKENS, HIDDEN)
    return pl.pallas_call(
        step_kernel,
        out_shape=outs(jax.ShapeDtypeStruct) + [
            jax.ShapeDtypeStruct((CHUNKS, 2, SPAN, WIDTH), bf16),
            jax.ShapeDtypeStruct((OWNED, WIDTH), f32),
            jax.ShapeDtypeStruct((2, TOKENS, WIDTH), bf16),
        ],
        in_specs=[anywhere] * 12,
        out_specs=[vmem] * 7,
        scratch_shapes=(
            shapes(CHUNKS)
            + shapes(CHUNKS)
            + shapes(CHUNKS)
            + shapes(PLANE)
            + shapes(2 * PLANE)
            + shapes(PLANE)
            + shapes(PLANE - 1)
            + [dma((len(STREAMS), SLOTS)), dma((len(STREAMS), SLOTS))]
            + [pltpu.VMEM((CHUNKS, 16, 512), f32), pltpu.VMEM((CHUNKS, 8, WIDTH), f32)]
            + [pltpu.VMEM(square, bf16)] * 3
            + [pltpu.VMEM((HIDDEN, WIDTH), bf16)]
            + [pltpu.VMEM(tokens, bf16)] * 4
            + [pltpu.VMEM(tokens, f32)] * 3
            + [pltpu.VMEM(tokens, bf16)] * 2
            + [
                pltpu.VMEM((TOKENS, WIDTH), bf16),
                pltpu.VMEM((OWNED, WIDTH), f32),
                pltpu.VMEM((WIDTH, OWNED), bf16),
                pltpu.VMEM((WIDTH, WIDTH), i32),
                pltpu.VMEM((CHUNKS, 8, WIDTH), i32),
                pltpu.VMEM((CHUNKS, 8, WIDTH), i32),
                pltpu.VMEM((2, 8, 8, WIDTH), i32),
                pltpu.VMEM((CHUNKS, SPAN, WIDTH), bf16),
                pltpu.VMEM((2, CHUNKS, SPAN, WIDTH), bf16),
                pltpu.VMEM((ROWBLOCK, ASKED), bf16),
                pltpu.VMEM((ROWBLOCK, ASKED), bf16),
                pltpu.VMEM((WIDTH, ASKED), f32),
                pltpu.VMEM((CHUNKS, SPAN, WIDTH), bf16),
                dma((12,)), dma((10,)), dma((10,)), dma((3,)), dma((3,)),
                pltpu.VMEM((1, 2 * SPAN, CHUNKS), i32),
                pltpu.VMEM((1, CHUNKS), i32),
                pltpu.VMEM((8, WIDTH), i32),
                pltpu.VMEM((8, WIDTH), i32),
                pltpu.VMEM((8, WIDTH), i32),
            ]
        ),
        compiler_params=pltpu.CompilerParams(
            collective_id=0, has_side_effects=True, vmem_limit_bytes=43 * 1024 * 1024
        ),
        name="step",
    )(*(pltpu.with_memory_space_constraint(a, pltpu.HBM) for a in args))


def deliver(results, factor):
    vmem = pl.BlockSpec(memory_space=pltpu.VMEM)
    pieces = 4

    def kernel(*refs):
        sources, targets, stages, sem = refs[:7], refs[7:14], refs[14:18], refs[18]
        copies = []

        def put(src, dst):
            c = pltpu.make_async_copy(src, dst, sem.at[len(copies)])
            c.start()
            copies.append(c)

        for src, dst in zip(sources[4:], targets[4:]):
            put(src, dst)
        for src, dst, stage in zip(sources, targets, stages):
            n = src.shape[0] // pieces
            for i in range(pieces):
                part = pl.ds(i * n, n)
                stage[part] = src[part].astype(f32) * factor
                put(stage.at[part], dst.at[part])
        for c in copies:
            c.wait()

    return pl.pallas_call(
        kernel,
        out_shape=[
            jax.ShapeDtypeStruct(r.shape, f32 if i < 4 else r.dtype) for i, r in enumerate(results)
        ],
        in_specs=[vmem] * 7,
        out_specs=[pl.BlockSpec(memory_space=pl.ANY)] * 7,
        scratch_shapes=[pltpu.VMEM(r.shape, f32) for r in results[:4]]
        + [pltpu.SemaphoreType.DMA((3 + 4 * pieces,))],
        compiler_params=pltpu.CompilerParams(vmem_limit_bytes=16 * 1024 * 1024),
        name="deliver",
    )(*results)


def local(
    hot_rows, hot_count, hot_cot, table, cold_ids, hash_mult, hash_add,
    layer_one, layer_two, layer_three, layer_four, cold_cot,
):
    results = step(
        hot_rows.transpose(0, 2, 1), hot_count, cold_ids.reshape(8, WIDTH),
        hash_mult.reshape(8, WIDTH), hash_add.reshape(8, WIDTH),
        layer_one, layer_two, layer_three, layer_four, cold_cot, hot_cot, table,
    )
    factor = float(cold_ids.shape[0] * lax.axis_size("dp")) ** (-0.5)
    g3, g4, g2, g1, hot_emb, new_table, cold_emb = deliver(results, factor)
    return (
        hot_emb.reshape(hot_cot.shape),
        new_table,
        cold_emb.reshape(cold_cot.shape),
        g1.reshape(layer_one.shape),
        g2.reshape(layer_two.shape),
        g3.reshape(layer_three.shape),
        g4.reshape(layer_four.shape),
    )


def solution(mesh):
    in_specs = (
        P("dp", None, None),
        P("dp", None),
        P("dp", None, None, None),
        P("dp", None),
        P("dp"),
        P(),
        P(),
        P(None, "mp"),
        P("mp", None),
        P(None, "mp"),
        P("mp", None),
        P("dp", None),
    )
    out_specs = (
        P("dp", None, None, None),
        P("dp", None),
        P("dp", None),
        P(None, "mp"),
        P("mp", None),
        P(None, "mp"),
        P("mp", None),
    )
    return jax.shard_map(local, mesh=mesh, in_specs=in_specs, out_specs=out_specs, check_vma=False)
```

```python
import jax
import jax.numpy as jnp
from jax import lax
from jax.experimental import pallas as pl
from jax.experimental.pallas import tpu as pltpu
from jax.sharding import PartitionSpec as P

MESH = pl.DeviceIdType.MESH
bf16, f32, i32 = jnp.bfloat16, jnp.float32, jnp.int32
learn_rate = 0.5
modulus = 1000003
RING = 4
PLANE = RING * RING
CHUNKS = RING * PLANE
HALF = PLANE // 2
TOKENS = 512
HIDDEN = 1024
MINE = 512
WIDTH = 128
OWNED = 4096
SPAN = 16
ASKED = CHUNKS * SPAN
ROWBLOCK = 512

THREE, FOUR, TWO, ONE = range(4)
LANES = (512, 128, 512, 512)
ROWS = (16, 8, 16, 16)
TYPES = (bf16,) * 4
DIRECT = (ONE,)
STREAMS = (
    (THREE, 0, 2, 0),
    (THREE, 2, 1, 1),
    (THREE, 3, 1, 2),
    (FOUR, 0, 1, 1),
    (TWO, 0, 2, 1),
    (TWO, 2, 1, 2),
    (TWO, 3, 1, 0),
    (ONE, 0, 2, 2),
    (ONE, 2, 1, 0),
    (ONE, 3, 1, 1),
)
SLOTS = 18


class Place:
    def __init__(self, axis):
        me = lax.axis_index("dp")
        self.core = lax.axis_index("mp")
        strides = (1, RING, RING * RING)
        self.stride = strides[axis]
        self.others = (strides[(axis + 1) % 3], strides[(axis + 2) % 3])
        self.k = lax.rem(lax.div(me, self.stride), RING)
        self.first = lax.rem(lax.div(me, self.others[0]), RING)
        self.second = lax.rem(lax.div(me, self.others[1]), RING)
        self.p = self.first * RING + self.second
        self.after = lax.rem(self.k + 1, RING)
        self.before = lax.rem(self.k + RING - 1, RING)
        self.opposite = lax.rem(self.k + 2, RING)
        self.right = me + (self.after - self.k) * self.stride
        self.left = me + (self.before - self.k) * self.stride

    def along(self, axis, j):
        at = self.second if axis else self.first
        to = lax.rem(at + j, RING)
        return lax.axis_index("dp") + (to - at) * self.others[axis], to

    def peer(self, p):
        return (
            self.k * self.stride
            + lax.div(p, RING) * self.others[0]
            + lax.rem(p, RING) * self.others[1]
        )


class Stream:
    def __init__(self, index, refs, places):
        self.grad, b0, nb, axis = STREAMS[index]
        self.place = places[axis]
        self.index = index
        self.lanes = pl.ds(b0 * WIDTH, nb * WIDTH)
        self.lane0, self.nlanes = b0 * WIDTH, nb * WIDTH
        g = self.grad
        for name in ("own", "other", "arrive", "total", "out", "near", "side", "part", "fan"):
            setattr(self, name, refs[name][g])
        self.send, self.recv = refs["send"], refs["recv"]
        self.dtype = TYPES[g]
        self.pending = []
        self.swaps = []

    def view(self, ref, first, count):
        return ref.at[pl.ds(first, count), :, self.lanes]

    def outview(self, ref, first, count):
        if self.grad != TWO:
            return self.view(ref, first, count)
        half = CHUNKS // 2
        lane = pl.multiple_of(lax.div(first, half) * 512 + self.lane0, WIDTH)
        return ref.at[pl.ds(lax.rem(first, half), count), :, pl.ds(lane, self.nlanes)]

    def load(self, ref, first, count):
        return ref[pl.ds(first, count), :, self.lanes].astype(f32)

    def store(self, ref, first, count, value):
        ref[pl.ds(first, count), :, self.lanes] = value.astype(self.dtype)

    def copy(self, src, dst, slot, device):
        return pltpu.make_async_remote_copy(
            src_ref=src, dst_ref=dst,
            send_sem=self.send.at[self.index, slot], recv_sem=self.recv.at[self.index, slot],
            device_id=device, device_id_type=MESH,
        )

    def start(self, src, dst, slot, dp=None, mp=None):
        where = (
            lax.axis_index("dp") if dp is None else dp,
            self.place.core if mp is None else mp,
        )
        c = self.copy(src, dst, slot, where)
        c.start()
        self.pending.append(c)
        return c

    def swap(self):
        self.swap_rows(0, CHUNKS, 0)

    def swap_low(self):
        self.swap_rows(0, CHUNKS // 2, 0)

    def swap_high(self):
        self.swap_rows(CHUNKS // 2, CHUNKS // 2, 17)

    def swap_rows(self, first, count, slot):
        self.swaps.append(self.start(
            self.view(self.other, first, count), self.view(self.arrive, first, count), slot,
            mp=1 - self.place.core,
        ))

    def combine(self):
        for c in self.swaps:
            c.wait_recv()

        @pl.loop(0, CHUNKS // 8, unroll=2)
        def _(i):
            self.store(
                self.total, i * 8, 8,
                self.load(self.own, i * 8, 8) + self.load(self.arrive, i * 8, 8),
            )

        q = self.place
        base = q.opposite * PLANE
        self.c_na = self.start(
            self.view(self.total, base, HALF), self.view(self.near, 0, HALF), 1, dp=q.right
        )
        self.c_nb = self.start(
            self.view(self.total, base + HALF, HALF), self.view(self.near, HALF, HALF), 2, dp=q.left
        )
        self.c_sa = self.start(
            self.view(self.total, q.after * PLANE + HALF, HALF),
            self.view(self.side, HALF, HALF), 3, dp=q.right,
        )
        self.c_sb = self.start(
            self.view(self.total, q.before * PLANE, HALF),
            self.view(self.side, PLANE, HALF), 4, dp=q.left,
        )

    def relay(self):
        q = self.place
        low, high = q.after * PLANE, q.before * PLANE + HALF
        self.c_na.wait_recv()
        self.store(
            self.total, low, HALF, self.load(self.total, low, HALF) + self.load(self.near, 0, HALF)
        )
        self.c_ra = self.start(
            self.view(self.total, low, HALF), self.view(self.side, 0, HALF), 5, dp=q.right
        )
        self.c_nb.wait_recv()
        self.store(
            self.total, high, HALF,
            self.load(self.total, high, HALF) + self.load(self.near, HALF, HALF),
        )
        self.c_rb = self.start(
            self.view(self.total, high, HALF), self.view(self.side, PLANE + HALF, HALF), 6, dp=q.left
        )

    def spread(self):
        q = self.place
        for c in (self.c_sa, self.c_sb, self.c_ra, self.c_rb):
            c.wait_recv()

        @pl.loop(0, PLANE // 4, unroll=2)
        def _(i):
            self.store(
                self.part, i * 4, 4,
                self.load(self.total, q.k * PLANE + i * 4, 4)
                + self.load(self.side, i * 4, 4)
                + self.load(self.side, PLANE + i * 4, 4),
            )

        if self.grad in DIRECT:
            @pl.loop(1, PLANE, unroll=5)
            def _(j):
                p = lax.rem(q.p + j, PLANE)
                self.copy(
                    self.view(self.part, p, 1), self.view(self.fan, j - 1, 1), 7, (q.peer(p), q.core)
                ).start()
        else:
            for j in range(1, RING):
                dp, to = q.along(0, j)
                self.copy(
                    self.view(self.part, to * RING, RING), self.view(self.fan, (j - 1) * RING, RING),
                    7, (dp, q.core),
                ).start()

    def middle(self):
        if self.grad in DIRECT:
            return
        q = self.place
        self.wait_chunks(7, 12, True)
        mine = q.first * RING
        acc = self.load(self.part, mine, RING)
        for j in range(3):
            acc = acc + self.load(self.fan, j * RING, RING)
        self.store(self.part, mine, RING, acc)
        for j in range(1, RING):
            dp, to = q.along(1, j)
            self.copy(
                self.view(self.part, mine + to, 1), self.view(self.fan, 11 + j, 1), 15, (dp, q.core)
            ).start()

    def wait_chunks(self, slot, count, recv):
        some = self.view(self.fan, 0, count)
        sem = (self.recv if recv else self.send).at[self.index, slot]
        pltpu.make_async_copy(some, some, sem).wait()

    def finish(self):
        q = self.place
        direct = self.grad in DIRECT
        if direct:
            self.wait_chunks(7, 15, True)
        else:
            self.wait_chunks(15, 3, True)
        acc = self.load(self.part, q.p, 1)
        for i in range(0 if direct else 12, PLANE - 1):
            acc = acc + self.load(self.fan, i, 1)
        here = q.k * PLANE + q.p
        result = self.outview(self.out, here, 1)
        result[...] = acc.astype(self.dtype)
        if direct:
            @pl.loop(1, PLANE, unroll=5)
            def _(j):
                p = lax.rem(q.p + j, PLANE)
                self.copy(result, result, 8, (q.peer(p), q.core)).start()
        else:
            for j in range(1, RING):
                self.copy(result, result, 8, (q.along(1, j)[0], q.core)).start()

    def collect(self):
        if self.grad in DIRECT:
            return
        q = self.place
        self.wait_chunks(8, 3, True)
        four = self.outview(self.out, q.k * PLANE + q.first * RING, RING)
        for j in range(1, RING):
            self.copy(four, four, 16, (q.along(0, j)[0], q.core)).start()

    def share(self):
        q = self.place
        if self.grad in DIRECT:
            self.wait_chunks(8, 15, True)
        else:
            self.wait_chunks(16, 12, True)
        low = self.outview(self.out, q.k * PLANE, HALF)
        high = self.outview(self.out, q.k * PLANE + HALF, HALF)
        self.c_gl = self.start(low, low, 9, dp=q.right)
        self.c_gh = self.start(high, high, 10, dp=q.left)
        self.c_hh = self.start(high, high, 11, dp=q.right)
        self.c_hl = self.start(low, low, 12, dp=q.left)

    def forward(self):
        q = self.place
        self.c_gl.wait_recv()
        low = self.outview(self.out, q.before * PLANE, HALF)
        self.c_fl = self.start(low, low, 13, dp=q.right)
        self.c_gh.wait_recv()
        high = self.outview(self.out, q.after * PLANE + HALF, HALF)
        self.c_fh = self.start(high, high, 14, dp=q.left)

    def close(self):
        for c in (self.c_hh, self.c_hl, self.c_fl, self.c_fh):
            c.wait_recv()

    def drain(self):
        for c in self.pending:
            c.wait_send()
        if self.grad in DIRECT:
            counts = ((7, 15), (8, 15))
        else:
            counts = ((7, 12), (15, 3), (8, 3), (16, 12))
        for slot, count in counts:
            self.wait_chunks(slot, count, False)


class Group:
    def __init__(self, streams):
        self.streams = streams

    def __getattr__(self, step):
        def run():
            for s in self.streams:
                getattr(s, step)()
        return run


def rows_by_columns(a, b):
    return lax.dot_general(a, b, (((0,), (0,)), ((), ())), preferred_element_type=f32)


def times_transposed(a, b):
    return lax.dot_general(a, b, (((1,), (1,)), ((), ())), preferred_element_type=f32)


def tile(n, size=256):
    return pl.ds(pl.multiple_of(n * size, size), size)


def step_kernel(
    rows_in, count_in, ids_in, mult_in, add_in, w1, w2, w3, w4, ccot, hcot, table,
    r3, r4, r2, r1, hout, newtab, emb,
    *rest,
):
    names = ("other", "arrive", "total", "near", "side", "part", "fan")
    refs = {name: rest[4 * i : 4 * i + 4] for i, name in enumerate(names)}
    rest = rest[4 * len(names) :]
    (
        refs["send"], refs["recv"], own_large, own_four,
        w1c, w2c, w3c, w4c, feats, a1, a2, a3, ds1, ds2, ds3, b2, b3, cot,
        tab, tabt, spare, rowmsg, rowbuf, rowsum, hc, carr, onehot, twohot, embt, ebuf,
        loads, wsend, wrecv, hsend, hrecv, rows, count, ids, mult, add,
    ) = rest
    b1 = b3
    refs["out"] = (r3, r4, r2, r1)
    refs["own"] = (own_large, own_four, own_large, own_large)
    me = lax.axis_index("dp")
    core = lax.axis_index("mp")
    partner = (me, 1 - core)
    places = [Place(a) for a in range(3)]
    streams = [Stream(i, refs, places) for i in range(len(STREAMS))]
    first, second, third = Group(streams[:4]), Group(streams[4:7]), Group(streams[7:])

    load = {}
    for n, (name, src, dst) in enumerate((
        ("rows", rows_in, rows),
        ("count", count_in, count),
        ("ids", ids_in, ids),
        ("mult", mult_in, mult),
        ("add", add_in, add),
        ("w1", w1, w1c.at[:, pl.ds(0, MINE)]),
        ("w2", w2, w2c.at[pl.ds(0, MINE)]),
        ("w3", w3, w3c.at[:, pl.ds(0, MINE)]),
        ("w4", w4, w4c.at[pl.ds(0, MINE)]),
        ("hcot", hcot.at[0, :, pl.ds(pl.multiple_of(core * SPAN, SPAN), SPAN)], hc),
        ("cot", ccot.at[pl.ds(pl.multiple_of(core * TOKENS, TOKENS), TOKENS)], cot),
        ("table", table, tab),
    )):
        load[name] = pltpu.make_async_copy(src, dst, loads.at[n])
        load[name].start()

    barrier = pltpu.get_barrier_semaphore()
    pl.semaphore_signal(barrier, inc=1, device_id=partner, device_id_type=MESH)

    @pl.loop(1, CHUNKS, unroll=7)
    def _(j):
        pl.semaphore_signal(
            barrier, inc=1, device_id=(lax.rem(me + j, CHUNKS), core), device_id_type=MESH
        )

    for name in ("rows", "count", "ids", "mult", "add"):
        load[name].wait()
    slot = lax.broadcasted_iota(i32, (SPAN, CHUNKS), 0) + core * SPAN
    want = rows[0, pl.ds(pl.multiple_of(core * SPAN, SPAN), SPAN), :] + 1
    spare[...] = jnp.zeros_like(spare)
    spare[pl.ds(pl.multiple_of(lax.rem(me, 8) * SPAN, SPAN), SPAN), pl.ds(0, CHUNKS)] = jnp.where(
        slot < count[...], want, 0
    )
    want = jnp.transpose(spare[...])[:CHUNKS]
    rowmsg[...] = jnp.broadcast_to(want[:, None, :], (CHUNKS, 8, WIDTH))

    def hash_block(b):
        line = ids[pl.ds(core * (TOKENS // WIDTH) + b, 1), :]
        column = jnp.transpose(jnp.broadcast_to(line, (WIDTH, WIDTH)))

        @pl.loop(0, HIDDEN // WIDTH, unroll=2)
        def _(j):
            h = column * mult[pl.ds(j, 1), :] + add[pl.ds(j, 1), :]
            q = (h.astype(f32) * ((1.0 - 4e-7) / modulus)).astype(i32)
            r = h - q * modulus
            r = jnp.where(r >= modulus, r - modulus, r)
            feats[pl.ds(b * WIDTH, WIDTH), tile(j, WIDTH)] = (
                r.astype(f32) * (2.0 / 1000002.0) - 1.0
            ).astype(bf16)

    hash_block(0)
    hash_block(1)
    pl.semaphore_wait(barrier, CHUNKS)

    sent = []

    def give(src, dst, n, device):
        c = pltpu.make_async_remote_copy(
            src_ref=src, dst_ref=dst, send_sem=wsend.at[n], recv_sem=wrecv.at[n],
            device_id=device, device_id_type=MESH,
        )
        c.start()
        sent.append(c)
        return c

    mine, theirs = pl.ds(0, MINE), pl.ds(MINE, MINE)
    load["w1"].wait()
    got1 = [
        give(w1c.at[:, pl.ds(256 * n, 256)], w1c.at[:, pl.ds(MINE + 256 * n, 256)], n, partner)
        for n in range(2)
    ]
    load["w2"].wait()
    got2 = give(w2c.at[mine], w2c.at[theirs], 9, partner)
    hash_block(2)
    hash_block(3)

    def hot_wait(ref, n, recv):
        sem = (hrecv if recv else hsend).at[n]
        part = ref.at[pl.ds(0, CHUNKS - 1)]
        pltpu.make_async_copy(part, part, sem).wait()

    def activate(pre, act, ds, rows, columns):
        sig = 0.5 * jnp.tanh(0.5 * pre) + 0.5
        act[rows, columns] = (pre * sig).astype(bf16)
        ds[rows, columns] = sig + (pre * sig) * (1.0 - sig)

    def layer(src, w, act, ds, lo, hi):
        last = None
        for n in range(lo, hi):
            for h in range(2):
                at = (pl.ds(h * 256, 256), pl.ds(n * 256, 256))
                pre = jnp.dot(src[at[0], :], w[:, at[1]], preferred_element_type=f32)
                if last is not None:
                    activate(last[0], act, ds, *last[1])
                last = (pre, at)
        activate(last[0], act, ds, *last[1])

    layer(feats, w1c, a1, ds1, 0, 2)
    load["w3"].wait()
    got3 = give(w3c.at[:, mine], w3c.at[:, theirs], 2, partner)
    load["w4"].wait()
    got4 = give(w4c.at[mine], w4c.at[theirs], 3, partner)
    load["table"].wait()

    @pl.loop(0, OWNED // WIDTH, unroll=8)
    def _(n):
        tabt[:, tile(n, WIDTH)] = jnp.transpose(tab[tile(n, WIDTH), :]).astype(bf16)

    got1[0].wait_recv()
    layer(feats, w1c, a1, ds1, 2, 3)
    got1[1].wait_recv()
    layer(feats, w1c, a1, ds1, 3, 4)

    load["hcot"].wait()

    def hot(src, dst, n, s):
        return pltpu.make_async_remote_copy(
            src_ref=src, dst_ref=dst, send_sem=hsend.at[n], recv_sem=hrecv.at[n],
            device_id=(s, core), device_id_type=MESH,
        )

    @pl.loop(1, CHUNKS, unroll=7)
    def _(j):
        o = lax.rem(me + j, CHUNKS)
        hot(rowmsg.at[o], rowbuf.at[me], 0, o).start()
        hot(hc.at[o], carr.at[0, me], 1, o).start()

    rowbuf[pl.ds(me, 1)] = rowmsg[pl.ds(me, 1)]
    carr[0, pl.ds(me, 1)] = hc[pl.ds(me, 1)]

    got2.wait_recv()
    layer(a1, w2c, a2, ds2, 0, 4)
    layer(a2, w3c, a3, ds3, 0, 2)
    got3.wait_recv()
    layer(a2, w3c, a3, ds3, 2, 4)
    got4.wait_recv()
    load["cot"].wait()

    def backward(src, w, ds, out):
        for n in range(4):
            columns = pl.ds(n * 256, 256)
            out[:, columns] = (times_transposed(src[...], w[columns, :]) * ds[:, columns]).astype(bf16)

    backward(cot, w4c, ds3, b3)

    def tall_grad(act, back, g, half, ref, lo=0, hi=4):
        for m in range(lo, hi):
            t = rows_by_columns(act[:, pl.ds(m * 256, 256)], back[:, pl.ds(half * MINE, MINE)])
            ref[g][pl.ds(m * 16, 16)] = t.reshape(16, 16, 512).astype(ref[g].dtype)

    def wide_grad(half, ref):
        for m in range(2):
            for h in range(2):
                t = rows_by_columns(a1[:, pl.ds((m + 2 * half) * 256, 256)], b2[:, pl.ds(h * 512, 512)])
                ref[TWO][pl.ds(h * 32 + m * 16, 16)] = t.reshape(16, 16, 512).astype(ref[TWO].dtype)

    def grad_four():
        t = rows_by_columns(cot[...], a3[...])
        for half, ref in ((1, other), (0, own)):
            part = jnp.transpose(t[:, half * MINE : (half + 1) * MINE])
            ref[FOUR][...] = part.reshape(CHUNKS, 8, WIDTH).astype(ref[FOUR].dtype)

    own, other = refs["own"], refs["other"]
    tall_grad(a2, b3, THREE, 1, other)
    Group(streams[:3]).swap()
    grad_four()
    streams[3].swap()
    tall_grad(a2, b3, THREE, 0, own)
    backward(b3, w3c, ds2, b2)
    first.combine()
    wide_grad(1, other)
    second.swap()
    wide_grad(0, own)
    backward(b2, w2c, ds1, b1)
    first.relay()
    second.combine()
    tall_grad(feats, b1, ONE, 1, other, 0, 2)
    third.swap_low()
    tall_grad(feats, b1, ONE, 1, other, 2, 4)
    third.swap_high()
    tall_grad(feats, b1, ONE, 0, own)

    emb[core] = jnp.dot(a3[...], w4c[...], preferred_element_type=f32).astype(bf16)
    got_emb = give(emb.at[core], emb.at[core], 4, partner)
    first.spread()
    second.relay()
    third.combine()

    hot_wait(rowbuf, 0, True)
    for g in range(8):
        total = rowbuf[8 * g]
        for i in range(1, 8):
            total = total + rowbuf[8 * g + i]
        rowsum[0, g] = total
    got_rows = give(rowsum.at[0], rowsum.at[1], 5, partner)
    hot_wait(carr.at[0], 1, True)
    got_carr = give(carr.at[0], carr.at[1], 6, partner)

    def select(which, block, into):
        row = lax.broadcasted_iota(i32, (ROWBLOCK, WIDTH), 0) + (block * ROWBLOCK + 1)
        for g in range(8):
            hit = row == jnp.broadcast_to(rowsum[which, g][0:1, :], (ROWBLOCK, WIDTH))
            into[:, pl.ds(g * WIDTH, WIDTH)] = jnp.where(hit, 1.0, 0.0).astype(bf16)

    blocks = OWNED // ROWBLOCK
    kept = core * (blocks // 2)

    def fetch(lo, hi, update):
        @pl.loop(lo, hi, step=2)
        def _(n):
            for k, hot_block in ((0, onehot), (1, twohot)):
                block = lax.rem(kept + n + k, blocks)
                where = tile(block, ROWBLOCK)
                select(0, block, hot_block)
                embt[...] += jnp.dot(tabt[:, where], hot_block[...], preferred_element_type=f32)
                if update:
                    delta = jnp.dot(
                        hot_block[...], carr[0].reshape(ASKED, WIDTH), preferred_element_type=f32
                    )
                    newtab[where, :] = tab[where, :] - learn_rate * delta

    def update(lo, hi):
        @pl.loop(lo, hi, step=2)
        def _(n):
            for k, hot_block in ((0, onehot), (1, twohot)):
                where = tile(kept + n + k, ROWBLOCK)
                select(1, kept + n + k, hot_block)
                delta = jnp.dot(
                    hot_block[...], carr[1].reshape(ASKED, WIDTH), preferred_element_type=f32
                )
                newtab[where, :] = newtab[where, :] - learn_rate * delta

    embt[...] = jnp.zeros_like(embt)
    fetch(0, 2, True)
    first.middle()
    second.spread()
    third.relay()
    fetch(2, 4, True)
    fetch(4, 6, False)
    first.finish()
    second.middle()
    third.spread()
    fetch(6, 8, False)

    for g in range(8):
        found = jnp.transpose(embt[:, pl.ds(g * WIDTH, WIDTH)]).astype(bf16)
        ebuf[pl.ds(g * 8, 8)] = found.reshape(8, SPAN, WIDTH)

    second.finish()
    first.collect()

    @pl.loop(1, CHUNKS, unroll=7)
    def _(j):
        s = lax.rem(me + j, CHUNKS)
        hot(ebuf.at[s], hout.at[me, core], 2, s).start()

    hout[pl.ds(me, 1), pl.ds(core, 1)] = ebuf[pl.ds(me, 1)][:, None]

    got_rows.wait_recv()
    got_carr.wait_recv()
    update(0, 2)
    third.finish()
    second.collect()
    first.share()
    update(2, 4)
    half = tile(core, OWNED // 2)
    got_table = give(newtab.at[half], newtab.at[half], 8, partner)
    second.share()
    first.forward()
    third.share()
    hot_wait(hout.at[:, 0], 2, True)
    got_hot = give(hout.at[:, core], hout.at[:, core], 7, partner)
    second.forward()
    third.forward()
    first.close()
    second.close()
    got_emb.wait_recv()
    got_table.wait_recv()
    got_hot.wait_recv()
    third.close()

    for group in (first, second, third):
        group.drain()
    for c in sent:
        c.wait_send()
    hot_wait(rowbuf, 0, False)
    hot_wait(carr.at[0], 1, False)
    hot_wait(ebuf, 2, False)


def shapes(count, types=TYPES):
    return [pltpu.VMEM((count, ROWS[g], LANES[g]), types[g]) for g in range(4)]


def outs(kind):
    sizes = [(CHUNKS, ROWS[g], LANES[g]) for g in range(4)]
    sizes[TWO] = (CHUNKS // 2, 16, 1024)
    return [kind(sizes[g], TYPES[g]) for g in range(4)]


def step(*args):
    vmem = pl.BlockSpec(memory_space=pltpu.VMEM)
    anywhere = pl.BlockSpec(memory_space=pl.ANY)
    dma = pltpu.SemaphoreType.DMA
    square = (HIDDEN, HIDDEN)
    tokens = (TOKENS, HIDDEN)
    return pl.pallas_call(
        step_kernel,
        out_shape=outs(jax.ShapeDtypeStruct) + [
            jax.ShapeDtypeStruct((CHUNKS, 2, SPAN, WIDTH), bf16),
            jax.ShapeDtypeStruct((OWNED, WIDTH), f32),
            jax.ShapeDtypeStruct((2, TOKENS, WIDTH), bf16),
        ],
        in_specs=[anywhere] * 12,
        out_specs=[vmem] * 7,
        scratch_shapes=(
            shapes(CHUNKS)
            + shapes(CHUNKS)
            + shapes(CHUNKS)
            + shapes(PLANE)
            + shapes(2 * PLANE)
            + shapes(PLANE)
            + shapes(PLANE - 1)
            + [dma((len(STREAMS), SLOTS)), dma((len(STREAMS), SLOTS))]
            + [pltpu.VMEM((CHUNKS, 16, 512), f32), pltpu.VMEM((CHUNKS, 8, WIDTH), f32)]
            + [pltpu.VMEM(square, bf16)] * 3
            + [pltpu.VMEM((HIDDEN, WIDTH), bf16)]
            + [pltpu.VMEM(tokens, bf16)] * 4
            + [pltpu.VMEM(tokens, f32)] * 3
            + [pltpu.VMEM(tokens, bf16)] * 2
            + [
                pltpu.VMEM((TOKENS, WIDTH), bf16),
                pltpu.VMEM((OWNED, WIDTH), f32),
                pltpu.VMEM((WIDTH, OWNED), bf16),
                pltpu.VMEM((WIDTH, WIDTH), i32),
                pltpu.VMEM((CHUNKS, 8, WIDTH), i32),
                pltpu.VMEM((CHUNKS, 8, WIDTH), i32),
                pltpu.VMEM((2, 8, 8, WIDTH), i32),
                pltpu.VMEM((CHUNKS, SPAN, WIDTH), bf16),
                pltpu.VMEM((2, CHUNKS, SPAN, WIDTH), bf16),
                pltpu.VMEM((ROWBLOCK, ASKED), bf16),
                pltpu.VMEM((ROWBLOCK, ASKED), bf16),
                pltpu.VMEM((WIDTH, ASKED), f32),
                pltpu.VMEM((CHUNKS, SPAN, WIDTH), bf16),
                dma((12,)), dma((10,)), dma((10,)), dma((3,)), dma((3,)),
                pltpu.VMEM((1, 2 * SPAN, CHUNKS), i32),
                pltpu.VMEM((1, CHUNKS), i32),
                pltpu.VMEM((8, WIDTH), i32),
                pltpu.VMEM((8, WIDTH), i32),
                pltpu.VMEM((8, WIDTH), i32),
            ]
        ),
        compiler_params=pltpu.CompilerParams(
            collective_id=0, has_side_effects=True, vmem_limit_bytes=43 * 1024 * 1024
        ),
        name="step",
    )(*(pltpu.with_memory_space_constraint(a, pltpu.HBM) for a in args))


def deliver(results, factor):
    vmem = pl.BlockSpec(memory_space=pltpu.VMEM)
    pieces = 4

    def kernel(*refs):
        sources, targets, stages, sem = refs[:7], refs[7:14], refs[14:18], refs[18]
        copies = []

        def put(src, dst):
            c = pltpu.make_async_copy(src, dst, sem.at[len(copies)])
            c.start()
            copies.append(c)

        for src, dst in zip(sources[4:], targets[4:]):
            put(src, dst)
        for src, dst, stage in zip(sources, targets, stages):
            n = src.shape[0] // pieces
            for i in range(pieces):
                part = pl.ds(i * n, n)
                stage[part] = src[part].astype(f32) * factor
                put(stage.at[part], dst.at[part])
        for c in copies:
            c.wait()

    return pl.pallas_call(
        kernel,
        out_shape=[
            jax.ShapeDtypeStruct(r.shape, f32 if i < 4 else r.dtype) for i, r in enumerate(results)
        ],
        in_specs=[vmem] * 7,
        out_specs=[pl.BlockSpec(memory_space=pl.ANY)] * 7,
        scratch_shapes=[pltpu.VMEM(r.shape, f32) for r in results[:4]]
        + [pltpu.SemaphoreType.DMA((3 + 4 * pieces,))],
        compiler_params=pltpu.CompilerParams(vmem_limit_bytes=16 * 1024 * 1024),
        name="deliver",
    )(*results)


def local(
    hot_rows, hot_count, hot_cot, table, cold_ids, hash_mult, hash_add,
    layer_one, layer_two, layer_three, layer_four, cold_cot,
):
    results = step(
        hot_rows.transpose(0, 2, 1), hot_count, cold_ids.reshape(8, WIDTH),
        hash_mult.reshape(8, WIDTH), hash_add.reshape(8, WIDTH),
        layer_one, layer_two, layer_three, layer_four, cold_cot, hot_cot, table,
    )
    factor = float(cold_ids.shape[0] * lax.axis_size("dp")) ** (-0.5)
    g3, g4, g2, g1, hot_emb, new_table, cold_emb = deliver(results, factor)
    return (
        hot_emb.reshape(hot_cot.shape),
        new_table,
        cold_emb.reshape(cold_cot.shape),
        g1.reshape(layer_one.shape),
        g2.reshape(layer_two.shape),
        g3.reshape(layer_three.shape),
        g4.reshape(layer_four.shape),
    )


def solution(mesh):
    in_specs = (
        P("dp", None, None),
        P("dp", None),
        P("dp", None, None, None),
        P("dp", None),
        P("dp"),
        P(),
        P(),
        P(None, "mp"),
        P("mp", None),
        P(None, "mp"),
        P("mp", None),
        P("dp", None),
    )
    out_specs = (
        P("dp", None, None, None),
        P("dp", None),
        P("dp", None),
        P(None, "mp"),
        P("mp", None),
        P(None, "mp"),
        P("mp", None),
    )
    return jax.shard_map(local, mesh=mesh, in_specs=in_specs, out_specs=out_specs, check_vma=False)
```
